32 devices in a mesh: grp: 2 (over y), dev: 16 (over z, x, core).
Axes of the slice: x: 2, y: 2, z: 4, core: 2. Of those that a mesh axis runs over, the one named last changes fastest.
Arguments:
- pooled_grad: bfloat16 [4096, 32, 128], P(('grp', 'dev')), may hold values from -6 to 6
- row_ids: int32 [4096, 4, 32], P(('grp', 'dev')), may hold values from 0 to 1023
- scale_exps: int32 [4096, 32], P(('grp', 'dev')), may hold values from 0 to 3
- table_owner: int32 [32], replicated, may hold values from 0 to 31, each once
- dense_acts: bfloat16 [4096, 512], P(('grp', 'dev')), may hold values from -6 to 6
- dense_cot: bfloat16 [4096, 512], P(('grp', 'dev')), may hold values from -0.1875 to 0.1875
Outputs:
- table_grad: float32 [32, 1024, 128], P('dev')
- weight_grad: float32 [512, 512], replicated
- bias_grad: float32 [512], replicated
The draws below stay inside these ranges and needn't reach their ends.
Inputs may be any that keep to these rules, and one draw needn't show every extreme that they name: Table t's rows are accumulated into slot table_owner[t]; each slot belongs to exactly one table.
All inputs are finite; a program needn't handle non-finite values.
Results may differ from the reference program's by a relative error of at most 0.0003.
Values may be sent and summed in bfloat16 or wider, within the bound.
A program may use at most 128 MiB of HBM per device.

```python
import jax
import jax.numpy as jnp
from jax import lax

E = 128
POOL = 4
HID = 512
HID2 = 512
ROWS = 1024
TABLES = 32
BATCH = 4096


def plant(array, own_key, smallest, top_value):
    longest = array.shape.index(max(array.shape))
    spots = []
    for shift in (0, 1):
        where = [jax.random.randint(jax.random.fold_in(own_key, axis), (), 0, length) for axis, length in enumerate(array.shape)]
        where[longest] = (where[longest] + shift) % array.shape[longest]
        spots.append(tuple(where))
    return array.at[spots[0]].set(smallest).at[spots[1]].set(top_value)


def raised(entries, stream_key, source, target, blocks, factor):
    def block_of(axis_at):
        return (jnp.arange(entries.shape[axis_at]) // (entries.shape[axis_at] // blocks)).reshape((-1,) + (1,) * (entries.ndim - 1 - axis_at))

    one_side = jax.random.permutation(stream_key, blocks)[block_of(target)]
    far = (block_of(target) + blocks // 2) % blocks
    return jnp.where((block_of(source) == one_side) | (block_of(source) == far), factor * entries, entries)


def shard_levels(key, dims, split, low, high):
    def one(position, blocks):
        steps = jax.random.uniform(jax.random.fold_in(jax.random.fold_in(key, 6), position), (blocks,), jnp.float32, low / len(split), high / len(split))
        return jnp.repeat(jnp.exp(steps), dims[position] // blocks).reshape((-1,) + (1,) * (len(dims) - position - 1))

    gain = one(*split[0])
    for cut in split[1:]:
        gain = gain * one(*cut)
    return gain


def normal_values(rng, extent, spread, most, pieces=(), kind=jnp.bfloat16):
    array = jax.random.normal(rng, extent, jnp.float32) * spread
    if len(pieces) > 0:
        array = shard_levels(rng, extent, pieces, -0.22, 0.18) * array
    return jnp.clip(array, min=-most, max=most).astype(kind)


def heavy_noise(key, extent, spread, bound, pieces, heavy, kind=jnp.bfloat16):
    array = spread * jax.random.normal(key, extent, jnp.float32)
    if pieces:
        array = array * shard_levels(key, extent, pieces, -0.22, 0.18)
    return jnp.clip(raised(array, jax.random.fold_in(key, 3), *heavy), -bound, bound).astype(kind)


def setup_inputs(seed: int = 0) -> dict:
    arg_keys = jax.random.split(jax.random.key(seed), 7)
    pooled_grad = normal_values(arg_keys[0], (BATCH, TABLES, E), 1.0, 6.0, ((0, 32),))
    row_ids = plant(jax.random.randint(arg_keys[1], (BATCH, POOL, TABLES), 0, ROWS), jax.random.fold_in(arg_keys[1], 1), 0, ROWS - 1).astype(jnp.int32)
    scale_exps = plant(jax.random.randint(arg_keys[2], (BATCH, TABLES), 0, 4), jax.random.fold_in(arg_keys[2], 1), 0, 3).astype(jnp.int32)
    table_owner = jax.random.permutation(arg_keys[3], TABLES).astype(jnp.int32)
    dense_acts = normal_values(arg_keys[4], (BATCH, HID), 1.0, 6.0, ((0, 32),))
    dense_cot = heavy_noise(arg_keys[5], (BATCH, HID2), BATCH ** -0.5, 0.1875, ((0, 32),), (0, 1, 32, 2.75))
    return dict(pooled_grad=pooled_grad, row_ids=row_ids, scale_exps=scale_exps, table_owner=table_owner, dense_acts=dense_acts, dense_cot=dense_cot)


def powers(exps):
    return (1.0 + (exps >= 1).astype(jnp.float32) + 2.0 * (exps >= 2).astype(jnp.float32)
            + 4.0 * (exps >= 3).astype(jnp.float32))


def reference(pooled_grad, row_ids, scale_exps, table_owner, dense_acts, dense_cot):
    factor = powers(scale_exps)
    quantized = jnp.clip(pooled_grad.astype(jnp.float32) / factor[:, :, None], -1.0, 1.0).astype(jnp.bfloat16)
    restored = (quantized.astype(jnp.float32) * factor[:, :, None]).astype(jnp.bfloat16)

    def per_table(column):
        values = jnp.take(restored, column, axis=1).astype(jnp.float32)
        indices = jnp.take(row_ids, column, axis=2).astype(jnp.int32)
        summed = jnp.zeros((ROWS, E), jnp.float32)
        for lookup in range(POOL):
            summed = summed.at[indices[:, lookup]].add(values)
        return summed

    by_table = lax.map(per_table, jnp.arange(TABLES, dtype=jnp.int32))
    table_grad = jnp.zeros_like(by_table).at[table_owner].set(by_table)
    weight_grad = lax.dot_general(dense_acts, dense_cot, (((0,), (0,)), ((), ())),
                                  preferred_element_type=jnp.float32)
    bias_grad = jnp.sum(dense_cot.astype(jnp.float32), axis=0)
    return table_grad, weight_grad, bias_grad
```

```python
import functools
import math

import jax
import jax.numpy as jnp
from jax import lax
from jax.experimental import pallas as pl
from jax.experimental.pallas import tpu as pltpu
from jax.sharding import PartitionSpec as P

ROWS = 1024
SPAN = 128
MESH = pl.DeviceIdType.MESH
CHUNKS = 4
PAD = 8
GROUP = 16
VMEM_MOST = 67043328
VMEM_SPARE = 8 << 20


def encode(ids):
    level = jnp.zeros(ids.shape, jnp.int32)
    scale = jnp.ones(ids.shape, jnp.float32)
    for k in range(1, ROWS // SPAN):
        level = jnp.where(ids >= k * SPAN, k, level)
        scale = jnp.where(ids >= k * SPAN, float(1 << k), scale)
    return (ids - level * SPAN + SPAN).astype(jnp.float32) * scale


def powers(exps):
    return (
        1.0
        + (exps >= 1).astype(jnp.float32)
        + 2.0 * (exps >= 2).astype(jnp.float32)
        + 4.0 * (exps >= 3).astype(jnp.float32)
    )


def kernel(
    devs,
    pool,
    owner_hbm,
    x_hbm,
    ids_hbm,
    exps_hbm,
    acts_hbm,
    cot_hbm,
    table_ref,
    whole,
    bias_ref,
    xv,
    xs,
    idv,
    exv,
    codes,
    base,
    owner_ref,
    slots,
    send,
    recv,
    inter,
    ga,
    gc,
    oa,
    oc,
    part,
    yh,
    zbuf,
    bp,
    bh,
    bz,
    bx,
    lsem,
    psend,
    precv,
    csend,
    crecv,
    fsend,
    frecv,
    isend,
    irecv,
    ysend,
    yrecv,
    zsend,
    zrecv,
    bsend,
    brecv,
    gsend,
    grecv,
    esend,
    erecv,
):
    me = lax.axis_index("dev")
    grp = lax.axis_index("grp")
    other = 1 - grp
    samples, tables, feat = x_hbm.shape
    owned = table_ref.shape[0]
    id_rows = owned * pool
    zs = devs // 4
    core = lax.rem(me, 2)
    xbit = lax.rem(lax.div(me, 2), 2)
    z = lax.div(me, 4)
    place = lax.rem(me, 4)
    tall, wide = oa.shape[1], oc.shape[1]
    cols = wide // 128
    half = part.shape[0] // 2
    piece = half // zs
    pitch = samples + PAD

    def remote(src, dst, ssem, rsem, dev, group):
        return pltpu.make_async_remote_copy(
            src_ref=src,
            dst_ref=dst,
            send_sem=ssem,
            recv_sem=rsem,
            device_id={"grp": group, "dev": dev},
            device_id_type=MESH,
        )

    places = (
        place,
        place + 1 - 2 * core,
        place + 2 - 4 * xbit,
        place + 3 - 4 * xbit - 2 * core,
    )
    near = z * 4 + places[1]
    across = z * 4 + places[2]

    def columns(ref, part_index, width):
        return ref.at[:, pl.ds(pl.multiple_of(part_index * width, 128), width)]

    def slot_rows(ref, index):
        return ref.at[pl.ds(pl.multiple_of(index * samples, 8), samples)]

    owner_load = pltpu.make_async_copy(owner_hbm, owner_ref, lsem.at[6 + CHUNKS])
    owner_load.start()
    loads = [
        pltpu.make_async_copy(columns(acts_hbm, core, tall), slot_rows(ga, place), lsem.at[0]),
        pltpu.make_async_copy(columns(cot_hbm, xbit, wide), slot_rows(gc, place), lsem.at[1]),
        pltpu.make_async_copy(columns(acts_hbm, 1 - core, tall), oa, lsem.at[2]),
        pltpu.make_async_copy(columns(cot_hbm, 1 - xbit, wide), oc, lsem.at[3]),
        pltpu.make_async_copy(exps_hbm, exv, lsem.at[4]),
        pltpu.make_async_copy(ids_hbm, idv, lsem.at[5]),
    ]
    step = samples // CHUNKS
    for c in range(CHUNKS):
        span = pl.ds(c * step, step)
        loads.append(pltpu.make_async_copy(x_hbm.at[span], xv.at[span], lsem.at[6 + c]))
    for load in loads:
        load.start()

    barrier = pltpu.get_barrier_semaphore()

    def greet(dev, group):
        pl.semaphore_signal(
            barrier, inc=1, device_id={"grp": group, "dev": dev}, device_id_type=MESH
        )

    for m in range(1, 4):
        greet(z * 4 + places[m], grp)

    @pl.loop(1, zs)
    def _(k):
        greet(lax.rem(z + k, zs) * 4 + place, grp)

    greet(me, other)

    base[...] = (
        (lax.broadcasted_iota(jnp.int32, base.shape, 0) + SPAN)
        .astype(jnp.float32)
        .astype(jnp.bfloat16)
    )

    owner_load.wait()

    @pl.loop(0, tables)
    def _(k):
        slots[k] = lax.fori_loop(
            0,
            tables,
            lambda t, found: jnp.maximum(found, (owner_ref[t] == k).astype(jnp.int32) * t),
            jnp.int32(0),
            unroll=16,
        )

    pl.semaphore_wait(barrier, 3 + zs)

    def plane_copies(m, slot):
        acts = oa if m in (1, 3) else slot_rows(ga, place)
        cots = oc if m in (2, 3) else slot_rows(gc, place)
        who = z * 4 + places[m]
        return (
            remote(
                acts, slot_rows(ga, slot), isend.at[2 * m - 2], irecv.at[2 * m - 2], who, grp
            ),
            remote(
                cots, slot_rows(gc, slot), isend.at[2 * m - 1], irecv.at[2 * m - 1], who, grp
            ),
        )

    for load in loads[:4]:
        load.wait()
    for m in (2, 3, 1):
        for copy in plane_copies(m, place):
            copy.start()

    loads[4].wait()
    loads[5].wait()
    for p in range(pool):
        codes.reshape(tables * 8, samples)[pl.ds(p, tables, stride=8), :] = encode(idv[p])

    flat = xs.reshape(tables * pitch, feat)
    for c in range(CHUNKS):
        loads[6 + c].wait()

        @pl.loop(0, tables // GROUP)
        def _(g):
            some = pl.ds(pl.multiple_of(g * GROUP, GROUP), GROUP)
            factor = powers(exv[some, :])
            first = g * (GROUP * pitch)
            for k in range(c * step, (c + 1) * step):
                bound = jnp.broadcast_to(factor[:, k : k + 1], (GROUP, feat))
                value = xv[k, some, :].astype(jnp.float32)
                rows = pl.ds(first + k, GROUP, stride=pitch)
                flat[rows, :] = jnp.clip(value, -bound, bound)

    def build(target, dst):
        picked = []
        for s in range(owned):
            t = slots[dst * owned + s]
            target[pl.ds(s * samples, samples), :] = xs[t][:samples].astype(jnp.bfloat16)
            picked.append(codes[t][:pool])
        target[pl.ds(owned * samples, id_rows), :] = jnp.concatenate(picked, axis=0).astype(
            jnp.bfloat16
        )

    def each_far(act):
        @pl.loop(1, zs)
        def _(i):
            for peer in (z + zs - i, z - zs + i):
                pl.when((peer >= 0) & (peer < zs))(functools.partial(act, peer))

    def each_near(act):
        @pl.loop(1, zs)
        def _(i):
            for peer in (z + i, z - i):
                pl.when((peer >= 0) & (peer < zs))(functools.partial(act, peer))

    def column_copy(m, peer):
        return remote(
            send.at[peer * 4 + places[m]],
            inter.at[m - 1, peer],
            psend.at[m - 1, peer],
            precv.at[m - 1, peer],
            z * 4 + places[m],
            grp,
        )

    def level_copy(m, back=False):
        who = z * 4 + places[m]
        return remote(
            send.at[who],
            recv.at[0, who if back else me],
            psend.at[m - 1, z],
            precv.at[m - 1, z],
            who,
            grp,
        )

    def line_copy(m, peer):
        origin = send.at[peer * 4 + place] if m == 0 else inter.at[m - 1, peer]
        return remote(
            origin,
            recv.at[0, z * 4 + places[m]],
            csend.at[m, peer],
            crecv.at[m, z],
            peer * 4 + place,
            grp,
        )

    def line_wait(m, peer):
        landing = recv.at[0, peer * 4 + places[m]]
        remote(
            landing, landing, csend.at[m, peer], crecv.at[m, peer], peer * 4 + place, grp
        ).wait_recv()

    def forward(src):
        return remote(
            recv.at[0, src], recv.at[1, src], fsend.at[src], frecv.at[src], me, other
        )

    def first_line(peer):
        dst = peer * 4 + place
        build(send.at[dst], dst)
        line_copy(0, peer).start()

    def column_start(m):
        def act(peer):
            dst = peer * 4 + places[m]
            build(send.at[dst], dst)
            column_copy(m, peer).start()

        each_far(act)
        build(send.at[z * 4 + places[m]], z * 4 + places[m])
        level_copy(m).start()

    def column_pass(m):
        def act(peer):
            column_copy(m, peer).wait_recv()
            line_copy(m, peer).start()

        each_far(act)

    def level_pass(m):
        level_copy(m, True).wait_recv()
        forward(z * 4 + places[m]).start()

    def line_pass(m):
        def act(peer):
            line_wait(m, peer)
            forward(peer * 4 + places[m]).start()

        each_near(act)

    def plane_finish():
        for m in range(1, 4):
            for copy in plane_copies(m, places[m]):
                copy.wait_recv()
        grad = lax.dot_general(
            ga[...], gc[...], (((0,), (0,)), ((), ())), preferred_element_type=jnp.float32
        )
        bias = jnp.sum(gc[...].astype(jnp.float32), axis=0, keepdims=True)
        bp[0] = jnp.zeros(bp.shape[1:], jnp.float32)
        for j in range(cols):
            part[pl.ds(j * tall, tall), :] = grad[:, j * 128 : (j + 1) * 128]
            bp[0, j : j + 1, :] = bias[:, j * 128 : (j + 1) * 128]

    def y_copies():
        away = part.at[pl.ds(pl.multiple_of(other * half, 8), half)]
        return (
            remote(away, yh, ysend.at[0], yrecv.at[0], me, other),
            remote(bp.at[0], bh, ysend.at[1], yrecv.at[1], me, other),
        )

    def y_start():
        for copy in y_copies():
            copy.start()

    def y_finish():
        for copy in y_copies():
            copy.wait()
        keep = pl.ds(pl.multiple_of(grp * half, 8), half)
        part[keep, :] = part[keep, :] + yh[...]
        bp[1] = bp[0] + bh[...]

    def piece_of(peer):
        return pl.ds(pl.multiple_of(grp * half + peer * piece, 8), piece)

    def z_copy(k, back=False):
        peer = lax.rem(z + k, zs)
        dev = peer * 4 + place
        origin, landing = (z, peer) if back else (peer, z)
        return (
            remote(
                part.at[piece_of(origin)],
                zbuf.at[landing],
                zsend.at[peer],
                zrecv.at[landing],
                dev,
                grp,
            ),
            remote(bp.at[1], bz.at[landing], bsend.at[peer], brecv.at[landing], dev, grp),
        )

    def z_start():
        @pl.loop(1, zs)
        def _(k):
            for copy in z_copy(k):
                copy.start()

    def z_finish():
        zbuf[z] = part[piece_of(z), :]
        bz[z] = bp[1]

        @pl.loop(1, zs)
        def _(k):
            for copy in z_copy(k, True):
                copy.wait_recv()

        whole[place, piece_of(z), :] = lax.fori_loop(
            1, zs, lambda i, run: run + zbuf[i], zbuf[0]
        )
        bp[2] = lax.fori_loop(1, zs, lambda i, run: run + bz[i], bz[0])

    def zg_copy(k, back=False):
        peer = lax.rem(z + k, zs)
        block = whole.at[place, piece_of(peer if back else z)]
        return remote(
            block, block, gsend.at[peer], grecv.at[peer if back else z], peer * 4 + place, grp
        )

    def bias_copy():
        return remote(bp.at[2], bx, bsend.at[zs], brecv.at[zs], across, grp)

    def zg_start():
        @pl.loop(1, zs)
        def _(k):
            zg_copy(k).start()

        bias_copy().start()

    def zg_finish():
        @pl.loop(1, zs)
        def _(k):
            zg_copy(k, True).wait_recv()

    halves = (grp, other)

    def tile_half(tile, which):
        return whole.at[tile, pl.ds(pl.multiple_of(which * half, 8), half)]

    def gather_copy(k, back=False):
        if k == 0:
            block = tile_half(place, other if back else grp)
            return remote(block, block, esend.at[0], erecv.at[0], me, other)
        if k < 3:
            block = tile_half(places[2] if back else place, halves[k - 1])
            return remote(block, block, esend.at[k], erecv.at[k], across, grp)
        if k < 5:
            block = tile_half(places[1] if back else place, halves[k - 3])
        else:
            block = tile_half(places[3] if back else places[2], halves[k - 5])
        return remote(block, block, esend.at[k], erecv.at[k], near, grp)

    def gather_start(*ks):
        for k in ks:
            gather_copy(k).start()

    def gather_wait(*ks):
        for k in ks:
            gather_copy(k, True).wait_recv()

    def accumulate(side, first, second):
        marks = jnp.concatenate(
            [
                recv[side, c, pl.ds(owned * samples, id_rows), :].astype(jnp.float32)
                for c in (first, second)
            ],
            axis=1,
        )
        one, zero = jnp.bfloat16(1), jnp.bfloat16(0)
        axis = base[...]
        for s in range(owned):
            values = jnp.concatenate(
                [recv[side, c, pl.ds(s * samples, samples), :] for c in (first, second)],
                axis=0,
            )
            rows = marks[s * pool : (s + 1) * pool]
            for block in range(ROWS // SPAN):
                local = (rows * (1.0 / (1 << block))).astype(jnp.bfloat16)
                counts = jnp.where(local[0:1] == axis, one, zero)
                for p in range(1, pool):
                    counts = counts + jnp.where(local[p : p + 1] == axis, one, zero)
                span = pl.ds(block * SPAN, SPAN)
                table_ref[s, span, :] = table_ref[s, span, :] + jnp.dot(
                    counts, values, preferred_element_type=jnp.float32
                )

    def pair(side, part_of, peer):
        accumulate(side, peer * 4 + places[2 * part_of], peer * 4 + places[2 * part_of + 1])

    def own_pairs(part_of):
        pair(0, part_of, z)
        each_near(functools.partial(pair, 0, part_of))

    def far_pair(part_of, peer):
        for m in (2 * part_of, 2 * part_of + 1):
            forward(peer * 4 + places[m]).wait_recv()
        pair(1, part_of, peer)

    each_far(first_line)
    build(recv.at[0, me], me)
    forward(me).start()
    column_start(1)
    column_start(2)
    column_start(3)
    column_pass(1)
    level_pass(1)
    table_ref[...] = jnp.zeros(table_ref.shape, jnp.float32)

    plane_finish()
    y_start()
    line_pass(0)
    y_finish()
    z_start()
    column_pass(2)
    level_pass(2)
    pair(0, 0, z)
    line_pass(1)
    z_finish()
    zg_start()
    column_pass(3)
    level_pass(3)
    each_near(functools.partial(pair, 0, 0))
    far_pair(0, z)
    line_pass(2)
    zg_finish()
    gather_start(0, 1, 3)
    pair(0, 1, z)
    each_near(functools.partial(far_pair, 0))
    gather_wait(0)
    gather_start(2, 4)
    line_pass(3)
    each_near(functools.partial(pair, 0, 1))
    gather_wait(1)
    gather_start(5)
    far_pair(1, z)
    gather_wait(2)
    gather_start(6)
    each_near(functools.partial(far_pair, 1))
    gather_wait(3, 4, 5, 6)


    bias_copy().wait_recv()
    mine, theirs = bp[2], bx[...]
    lower = jnp.where(xbit == 0, mine, theirs)
    upper = jnp.where(xbit == 0, theirs, mine)
    for j in range(cols):
        bias_ref[:, j * 128 : (j + 1) * 128] = lower[j : j + 1, :]
        bias_ref[:, (cols + j) * 128 : (cols + j + 1) * 128] = upper[j : j + 1, :]

    bias_copy().wait_send()
    for k in range(7):
        gather_copy(k).wait_send()
    for m in range(1, 4):
        level_copy(m).wait_send()
        for copy in plane_copies(m, place):
            copy.wait_send()

    @pl.loop(1, zs)
    def _(k):
        for copy in z_copy(k):
            copy.wait_send()
        zg_copy(k).wait_send()

    def drain(peer):
        for m in range(4):
            line_copy(m, peer).wait_send()
            if m > 0:
                column_copy(m, peer).wait_send()

    each_near(drain)

    @pl.loop(0, devs)
    def _(src):
        forward(src).wait_send()


def place_outputs(table_in, whole_in, bias_in, table_out, weight_out, bias_out, sems):
    tiles, rows, _ = whole_in.shape
    tall = weight_out.shape[0] // 2
    cols = rows // tall
    copies = []
    for s in range(table_in.shape[0]):
        copies.append((table_in.at[s], table_out.at[s]))
    for tile in range(tiles):
        for j in range(cols):
            block = (tile // 2) * cols + j
            copies.append(
                (
                    whole_in.at[tile, pl.ds(j * tall, tall)],
                    weight_out.at[pl.ds((tile % 2) * tall, tall), pl.ds(block * 128, 128)],
                )
            )
    copies.append((bias_in, bias_out))
    started = [
        pltpu.make_async_copy(src, dst, sems.at[i]) for i, (src, dst) in enumerate(copies)
    ]
    for copy in started:
        copy.start()
    for copy in started:
        copy.wait()


def solution(mesh):
    devs = mesh.shape["dev"]

    def per_device(pooled_grad, row_ids, scale_exps, table_owner, dense_acts, dense_cot):
        samples, tables, feat = pooled_grad.shape
        pool = row_ids.shape[1]
        owned = tables // devs
        hid, hid2 = dense_acts.shape[1], dense_cot.shape[1]
        tall, wide = hid // 2, hid2 // 2
        zs = devs // 4
        rows = owned * (samples + pool)
        total = tall * wide // 128
        half = total // 2
        dma = pltpu.SemaphoreType.DMA
        vmem = pl.BlockSpec(memory_space=pltpu.VMEM)
        hbm = pl.BlockSpec(memory_space=pltpu.HBM)
        f32, bf16, i32 = jnp.float32, jnp.bfloat16, jnp.int32
        buffers = [
            pltpu.VMEM((samples, tables, feat), bf16),
            pltpu.VMEM((tables, samples + PAD, feat), f32),
            pltpu.VMEM((pool, tables, samples), i32),
            pltpu.VMEM((tables, samples), i32),
            pltpu.VMEM((tables, 8, samples), f32),
            pltpu.VMEM((SPAN, 2 * samples), bf16),
            pltpu.VMEM((devs, rows, feat), bf16),
            pltpu.VMEM((2, devs, rows, feat), bf16),
            pltpu.VMEM((3, zs, rows, feat), bf16),
            pltpu.VMEM((4 * samples, tall), bf16),
            pltpu.VMEM((4 * samples, wide), bf16),
            pltpu.VMEM((samples, tall), bf16),
            pltpu.VMEM((samples, wide), bf16),
            pltpu.VMEM((total, 128), f32),
            pltpu.VMEM((half, 128), f32),
            pltpu.VMEM((zs, half // zs, 128), f32),
            pltpu.VMEM((3, 8, 128), f32),
            pltpu.VMEM((8, 128), f32),
            pltpu.VMEM((zs, 8, 128), f32),
            pltpu.VMEM((8, 128), f32),
        ]
        held = sum(math.prod(b.shape) * jnp.dtype(b.dtype).itemsize for b in buffers)
        partial = pl.pallas_call(
            functools.partial(kernel, devs, pool),
            out_shape=(
                jax.ShapeDtypeStruct((owned, ROWS, feat), f32),
                jax.ShapeDtypeStruct((4, total, 128), f32),
                jax.ShapeDtypeStruct((1, hid2), f32),
            ),
            in_specs=[hbm] * 6,
            out_specs=(vmem, vmem, vmem),
            scratch_shapes=buffers[:6]
            + [pltpu.SMEM((tables,), i32)] * 2
            + buffers[6:]
            + [
                dma((7 + CHUNKS,)),
                dma((3, zs)),
                dma((3, zs)),
                dma((4, zs)),
                dma((4, zs)),
                dma((devs,)),
                dma((devs,)),
                dma((6,)),
                dma((6,)),
                dma((2,)),
                dma((2,)),
                dma((zs,)),
                dma((zs,)),
                dma((zs + 1,)),
                dma((zs + 1,)),
                dma((zs,)),
                dma((zs,)),
                dma((7,)),
                dma((7,)),
            ],
            compiler_params=pltpu.CompilerParams(
                collective_id=0,
                has_side_effects=True,
                vmem_limit_bytes=min(held + VMEM_SPARE, VMEM_MOST),
            ),
        )(
            pltpu.with_memory_space_constraint(table_owner, pltpu.HBM),
            pltpu.with_memory_space_constraint(pooled_grad, pltpu.HBM),
            pltpu.with_memory_space_constraint(jnp.transpose(row_ids, (1, 2, 0)), pltpu.HBM),
            pltpu.with_memory_space_constraint(jnp.transpose(scale_exps, (1, 0)), pltpu.HBM),
            pltpu.with_memory_space_constraint(dense_acts, pltpu.HBM),
            pltpu.with_memory_space_constraint(dense_cot, pltpu.HBM),
        )
        cols = total // tall
        table_grad, weight_grad, bias_grad = pl.pallas_call(
            place_outputs,
            out_shape=(
                jax.ShapeDtypeStruct((owned, ROWS, feat), f32),
                jax.ShapeDtypeStruct((hid, hid2), f32),
                jax.ShapeDtypeStruct((1, hid2), f32),
            ),
            in_specs=[vmem] * 3,
            out_specs=(hbm, hbm, hbm),
            scratch_shapes=[dma((owned + 4 * cols + 1,))],
            compiler_params=pltpu.CompilerParams(vmem_limit_bytes=16 << 20),
        )(*partial)
        return table_grad, weight_grad, bias_grad.reshape(hid2)

    return jax.shard_map(
        per_device,
        mesh=mesh,
        in_specs=(
            P(("grp", "dev"), None, None),
            P(("grp", "dev"), None, None),
            P(("grp", "dev"), None),
            P(),
            P(("grp", "dev"), None),
            P(("grp", "dev"), None),
        ),
        out_specs=(P("dev", None, None), P(), P()),
        check_vma=False,
    )
```

```python
import functools
import math

import jax
import jax.numpy as jnp
from jax import lax
from jax.experimental import pallas as pl
from jax.experimental.pallas import tpu as pltpu
from jax.sharding import PartitionSpec as P

ROWS = 1024
SPAN = 128
MESH = pl.DeviceIdType.MESH
CHUNKS = 4
PAD = 8
GROUP = 16
VMEM_MOST = 67043328
VMEM_SPARE = 8 << 20


def encode(ids):
    level = jnp.zeros(ids.shape, jnp.int32)
    scale = jnp.ones(ids.shape, jnp.float32)
    for k in range(1, ROWS // SPAN):
        level = jnp.where(ids >= k * SPAN, k, level)
        scale = jnp.where(ids >= k * SPAN, float(1 << k), scale)
    return (ids - level * SPAN + SPAN).astype(jnp.float32) * scale


def powers(exps):
    return (
        1.0
        + (exps >= 1).astype(jnp.float32)
        + 2.0 * (exps >= 2).astype(jnp.float32)
        + 4.0 * (exps >= 3).astype(jnp.float32)
    )


def kernel(
    devs,
    pool,
    owner_hbm,
    x_hbm,
    ids_hbm,
    exps_hbm,
    acts_hbm,
    cot_hbm,
    table_ref,
    whole,
    bias_ref,
    xv,
    xs,
    idv,
    exv,
    codes,
    base,
    owner_ref,
    slots,
    send,
    recv,
    inter,
    ga,
    gc,
    oa,
    oc,
    part,
    yh,
    zbuf,
    bp,
    bh,
    bz,
    bx,
    lsem,
    psend,
    precv,
    csend,
    crecv,
    fsend,
    frecv,
    isend,
    irecv,
    ysend,
    yrecv,
    zsend,
    zrecv,
    bsend,
    brecv,
    gsend,
    grecv,
    esend,
    erecv,
):
    me = lax.axis_index("dev")
    grp = lax.axis_index("grp")
    other = 1 - grp
    samples, tables, feat = x_hbm.shape
    owned = table_ref.shape[0]
    id_rows = owned * pool
    zs = devs // 4
    core = lax.rem(me, 2)
    xbit = lax.rem(lax.div(me, 2), 2)
    z = lax.div(me, 4)
    place = lax.rem(me, 4)
    tall, wide = oa.shape[1], oc.shape[1]
    cols = wide // 128
    half = part.shape[0] // 2
    piece = half // zs
    pitch = samples + PAD

    def remote(src, dst, ssem, rsem, dev, group):
        return pltpu.make_async_remote_copy(
            src_ref=src,
            dst_ref=dst,
            send_sem=ssem,
            recv_sem=rsem,
            device_id={"grp": group, "dev": dev},
            device_id_type=MESH,
        )

    places = (
        place,
        place + 1 - 2 * core,
        place + 2 - 4 * xbit,
        place + 3 - 4 * xbit - 2 * core,
    )
    near = z * 4 + places[1]
    across = z * 4 + places[2]

    def columns(ref, part_index, width):
        return ref.at[:, pl.ds(pl.multiple_of(part_index * width, 128), width)]

    def slot_rows(ref, index):
        return ref.at[pl.ds(pl.multiple_of(index * samples, 8), samples)]

    owner_load = pltpu.make_async_copy(owner_hbm, owner_ref, lsem.at[6 + CHUNKS])
    owner_load.start()
    loads = [
        pltpu.make_async_copy(columns(acts_hbm, core, tall), slot_rows(ga, place), lsem.at[0]),
        pltpu.make_async_copy(columns(cot_hbm, xbit, wide), slot_rows(gc, place), lsem.at[1]),
        pltpu.make_async_copy(columns(acts_hbm, 1 - core, tall), oa, lsem.at[2]),
        pltpu.make_async_copy(columns(cot_hbm, 1 - xbit, wide), oc, lsem.at[3]),
        pltpu.make_async_copy(exps_hbm, exv, lsem.at[4]),
        pltpu.make_async_copy(ids_hbm, idv, lsem.at[5]),
    ]
    step = samples // CHUNKS
    for c in range(CHUNKS):
        span = pl.ds(c * step, step)
        loads.append(pltpu.make_async_copy(x_hbm.at[span], xv.at[span], lsem.at[6 + c]))
    for load in loads:
        load.start()

    barrier = pltpu.get_barrier_semaphore()

    def greet(dev, group):
        pl.semaphore_signal(
            barrier, inc=1, device_id={"grp": group, "dev": dev}, device_id_type=MESH
        )

    for m in range(1, 4):
        greet(z * 4 + places[m], grp)

    @pl.loop(1, zs)
    def _(k):
        greet(lax.rem(z + k, zs) * 4 + place, grp)

    greet(me, other)

    base[...] = (
        (lax.broadcasted_iota(jnp.int32, base.shape, 0) + SPAN)
        .astype(jnp.float32)
        .astype(jnp.bfloat16)
    )

    owner_load.wait()

    @pl.loop(0, tables)
    def _(k):
        slots[k] = lax.fori_loop(
            0,
            tables,
            lambda t, found: jnp.maximum(found, (owner_ref[t] == k).astype(jnp.int32) * t),
            jnp.int32(0),
            unroll=16,
        )

    pl.semaphore_wait(barrier, 3 + zs)

    def plane_copies(m, slot):
        acts = oa if m in (1, 3) else slot_rows(ga, place)
        cots = oc if m in (2, 3) else slot_rows(gc, place)
        who = z * 4 + places[m]
        return (
            remote(
                acts, slot_rows(ga, slot), isend.at[2 * m - 2], irecv.at[2 * m - 2], who, grp
            ),
            remote(
                cots, slot_rows(gc, slot), isend.at[2 * m - 1], irecv.at[2 * m - 1], who, grp
            ),
        )

    for load in loads[:4]:
        load.wait()
    for m in (2, 3, 1):
        for copy in plane_copies(m, place):
            copy.start()

    loads[4].wait()
    loads[5].wait()
    for p in range(pool):
        codes.reshape(tables * 8, samples)[pl.ds(p, tables, stride=8), :] = encode(idv[p])

    flat = xs.reshape(tables * pitch, feat)
    for c in range(CHUNKS):
        loads[6 + c].wait()

        @pl.loop(0, tables // GROUP)
        def _(g):
            some = pl.ds(pl.multiple_of(g * GROUP, GROUP), GROUP)
            factor = powers(exv[some, :])
            first = g * (GROUP * pitch)
            for k in range(c * step, (c + 1) * step):
                bound = jnp.broadcast_to(factor[:, k : k + 1], (GROUP, feat))
                value = xv[k, some, :].astype(jnp.float32)
                rows = pl.ds(first + k, GROUP, stride=pitch)
                flat[rows, :] = jnp.clip(value, -bound, bound)

    def build(target, dst):
        picked = []
        for s in range(owned):
            t = slots[dst * owned + s]
            target[pl.ds(s * samples, samples), :] = xs[t][:samples].astype(jnp.bfloat16)
            picked.append(codes[t][:pool])
        target[pl.ds(owned * samples, id_rows), :] = jnp.concatenate(picked, axis=0).astype(
            jnp.bfloat16
        )

    def each_near(act, first=1, last=zs):
        @pl.loop(first, last)
        def _(i):
            @pl.loop(0, 2)
            def _(j):
                peer = z + i * (1 - 2 * j)
                pl.when((peer >= 0) & (peer < zs))(functools.partial(act, peer))

    def close(act):
        each_near(act, 1, 2)

    def rest(act):
        each_near(act, 2, zs)

    def column_copy(m, peer):
        return remote(
            send.at[peer * 4 + places[m]],
            inter.at[m - 1, peer],
            psend.at[m - 1, peer],
            precv.at[m - 1, peer],
            z * 4 + places[m],
            grp,
        )

    def level_copy(m, back=False):
        who = z * 4 + places[m]
        return remote(
            send.at[who],
            recv.at[0, who if back else me],
            psend.at[m - 1, z],
            precv.at[m - 1, z],
            who,
            grp,
        )

    def line_copy(m, peer):
        origin = send.at[peer * 4 + place] if m == 0 else inter.at[m - 1, peer]
        return remote(
            origin,
            recv.at[0, z * 4 + places[m]],
            csend.at[m, peer],
            crecv.at[m, z],
            peer * 4 + place,
            grp,
        )

    def line_wait(m, peer):
        landing = recv.at[0, peer * 4 + places[m]]
        remote(
            landing, landing, csend.at[m, peer], crecv.at[m, peer], peer * 4 + place, grp
        ).wait_recv()

    def forward(src):
        return remote(
            recv.at[0, src], recv.at[1, src], fsend.at[src], frecv.at[src], me, other
        )

    def first_line(peer):
        dst = peer * 4 + place
        build(send.at[dst], dst)
        line_copy(0, peer).start()

    def column_start(m):
        def act(peer):
            dst = peer * 4 + places[m]
            build(send.at[dst], dst)
            column_copy(m, peer).start()

        each_near(act)

    def level_start(m):
        build(send.at[z * 4 + places[m]], z * 4 + places[m])
        level_copy(m).start()

    def column_pass(m, each):
        def act(peer):
            column_copy(m, peer).wait_recv()
            line_copy(m, peer).start()

        each(act)

    def level_pass(m):
        level_copy(m, True).wait_recv()
        forward(z * 4 + places[m]).start()

    def line_pass(m, each):
        def act(peer):
            line_wait(m, peer)
            forward(peer * 4 + places[m]).start()

        each(act)

    def plane_finish():
        for m in range(1, 4):
            for copy in plane_copies(m, places[m]):
                copy.wait_recv()
        grad = lax.dot_general(
            ga[...], gc[...], (((0,), (0,)), ((), ())), preferred_element_type=jnp.float32
        )
        bias = jnp.sum(gc[...].astype(jnp.float32), axis=0, keepdims=True)
        bp[0] = jnp.zeros(bp.shape[1:], jnp.float32)
        for j in range(cols):
            part[pl.ds(j * tall, tall), :] = grad[:, j * 128 : (j + 1) * 128]
            bp[0, j : j + 1, :] = bias[:, j * 128 : (j + 1) * 128]

    def y_copies():
        away = part.at[pl.ds(pl.multiple_of(other * half, 8), half)]
        return (
            remote(away, yh, ysend.at[0], yrecv.at[0], me, other),
            remote(bp.at[0], bh, ysend.at[1], yrecv.at[1], me, other),
        )

    def y_start():
        for copy in y_copies():
            copy.start()

    def y_finish():
        for copy in y_copies():
            copy.wait()
        keep = pl.ds(pl.multiple_of(grp * half, 8), half)
        part[keep, :] = part[keep, :] + yh[...]
        bp[1] = bp[0] + bh[...]

    def piece_of(peer):
        return pl.ds(pl.multiple_of(grp * half + peer * piece, 8), piece)

    def z_copy(k, back=False):
        peer = lax.rem(z + k, zs)
        dev = peer * 4 + place
        origin, landing = (z, peer) if back else (peer, z)
        return (
            remote(
                part.at[piece_of(origin)],
                zbuf.at[landing],
                zsend.at[peer],
                zrecv.at[landing],
                dev,
                grp,
            ),
            remote(bp.at[1], bz.at[landing], bsend.at[peer], brecv.at[landing], dev, grp),
        )

    def z_start():
        @pl.loop(1, zs)
        def _(k):
            for copy in z_copy(k):
                copy.start()

    def z_finish():
        zbuf[z] = part[piece_of(z), :]
        bz[z] = bp[1]

        @pl.loop(1, zs)
        def _(k):
            for copy in z_copy(k, True):
                copy.wait_recv()

        whole[place, piece_of(z), :] = lax.fori_loop(
            1, zs, lambda i, run: run + zbuf[i], zbuf[0]
        )
        bp[2] = lax.fori_loop(1, zs, lambda i, run: run + bz[i], bz[0])

    def zg_copy(k, back=False):
        peer = lax.rem(z + k, zs)
        block = whole.at[place, piece_of(peer if back else z)]
        return remote(
            block, block, gsend.at[peer], grecv.at[peer if back else z], peer * 4 + place, grp
        )

    def bias_copy():
        return remote(bp.at[2], bx, bsend.at[zs], brecv.at[zs], across, grp)

    def zg_start():
        @pl.loop(1, zs)
        def _(k):
            zg_copy(k).start()

        bias_copy().start()

    def zg_finish():
        @pl.loop(1, zs)
        def _(k):
            zg_copy(k, True).wait_recv()

    halves = (grp, other)

    def tile_half(tile, which):
        return whole.at[tile, pl.ds(pl.multiple_of(which * half, 8), half)]

    def gather_copy(k, back=False):
        if k == 0:
            block = tile_half(place, other if back else grp)
            return remote(block, block, esend.at[0], erecv.at[0], me, other)
        if k < 3:
            block = tile_half(places[2] if back else place, halves[k - 1])
            return remote(block, block, esend.at[k], erecv.at[k], across, grp)
        if k < 5:
            block = tile_half(places[1] if back else place, halves[k - 3])
        else:
            block = tile_half(places[3] if back else places[2], halves[k - 5])
        return remote(block, block, esend.at[k], erecv.at[k], near, grp)

    def gather_start(*ks):
        for k in ks:
            gather_copy(k).start()

    def gather_wait(*ks):
        for k in ks:
            gather_copy(k, True).wait_recv()

    def accumulate(side, first, second):
        marks = jnp.concatenate(
            [
                recv[side, c, pl.ds(owned * samples, id_rows), :].astype(jnp.float32)
                for c in (first, second)
            ],
            axis=1,
        )
        one, zero = jnp.bfloat16(1), jnp.bfloat16(0)
        axis = base[...]
        for s in range(owned):
            values = jnp.concatenate(
                [recv[side, c, pl.ds(s * samples, samples), :] for c in (first, second)],
                axis=0,
            )
            rows = marks[s * pool : (s + 1) * pool]
            for block in range(ROWS // SPAN):
                local = (rows * (1.0 / (1 << block))).astype(jnp.bfloat16)
                counts = jnp.where(local[0:1] == axis, one, zero)
                for p in range(1, pool):
                    counts = counts + jnp.where(local[p : p + 1] == axis, one, zero)
                span = pl.ds(block * SPAN, SPAN)
                table_ref[s, span, :] = table_ref[s, span, :] + jnp.dot(
                    counts, values, preferred_element_type=jnp.float32
                )

    def pair(side, part_of, peer):
        accumulate(side, peer * 4 + places[2 * part_of], peer * 4 + places[2 * part_of + 1])

    def far_pair(part_of, peer):
        for m in (2 * part_of, 2 * part_of + 1):
            forward(peer * 4 + places[m]).wait_recv()
        pair(1, part_of, peer)

    each_near(first_line)
    build(recv.at[0, me], me)
    forward(me).start()
    level_start(1)
    level_start(2)
    level_start(3)
    column_start(1)
    column_start(2)
    column_start(3)
    column_pass(1, close)
    column_pass(1, rest)
    level_pass(1)
    table_ref[...] = jnp.zeros(table_ref.shape, jnp.float32)
    plane_finish()
    y_start()
    line_pass(0, close)
    y_finish()
    z_start()
    level_pass(2)
    level_pass(3)
    line_pass(0, rest)
    column_pass(2, close)
    pair(0, 0, z)
    line_pass(1, close)
    z_finish()
    zg_start()
    column_pass(2, rest)
    line_pass(1, rest)
    column_pass(3, close)
    column_pass(3, rest)
    close(functools.partial(pair, 0, 0))
    rest(functools.partial(pair, 0, 0))
    far_pair(0, z)
    line_pass(2, close)
    zg_finish()
    gather_start(0, 1, 3)
    line_pass(2, rest)
    pair(0, 1, z)
    close(functools.partial(far_pair, 0))
    rest(functools.partial(far_pair, 0))
    gather_wait(0)
    gather_start(2, 4)
    line_pass(3, close)
    line_pass(3, rest)
    close(functools.partial(pair, 0, 1))
    rest(functools.partial(pair, 0, 1))
    gather_wait(1)
    gather_start(5)
    far_pair(1, z)
    gather_wait(2)
    gather_start(6)
    close(functools.partial(far_pair, 1))
    rest(functools.partial(far_pair, 1))
    gather_wait(3, 4)
    gather_wait(5, 6)

    bias_copy().wait_recv()
    mine, theirs = bp[2], bx[...]
    lower = jnp.where(xbit == 0, mine, theirs)
    upper = jnp.where(xbit == 0, theirs, mine)
    for j in range(cols):
        bias_ref[:, j * 128 : (j + 1) * 128] = lower[j : j + 1, :]
        bias_ref[:, (cols + j) * 128 : (cols + j + 1) * 128] = upper[j : j + 1, :]

    bias_copy().wait_send()
    for k in range(7):
        gather_copy(k).wait_send()
    for m in range(1, 4):
        level_copy(m).wait_send()
        for copy in plane_copies(m, place):
            copy.wait_send()

    @pl.loop(1, zs)
    def _(k):
        for copy in z_copy(k):
            copy.wait_send()
        zg_copy(k).wait_send()

    def drain(peer):
        for m in range(4):
            line_copy(m, peer).wait_send()
            if m > 0:
                column_copy(m, peer).wait_send()

    each_near(drain)

    @pl.loop(0, devs)
    def _(src):
        forward(src).wait_send()


def place_outputs(table_in, whole_in, bias_in, table_out, weight_out, bias_out, sems):
    tiles, rows, _ = whole_in.shape
    tall = weight_out.shape[0] // 2
    cols = rows // tall
    copies = []
    for s in range(table_in.shape[0]):
        copies.append((table_in.at[s], table_out.at[s]))
    for tile in range(tiles):
        for j in range(cols):
            block = (tile // 2) * cols + j
            copies.append(
                (
                    whole_in.at[tile, pl.ds(j * tall, tall)],
                    weight_out.at[pl.ds((tile % 2) * tall, tall), pl.ds(block * 128, 128)],
                )
            )
    copies.append((bias_in, bias_out))
    started = [
        pltpu.make_async_copy(src, dst, sems.at[i]) for i, (src, dst) in enumerate(copies)
    ]
    for copy in started:
        copy.start()
    for copy in started:
        copy.wait()


def solution(mesh):
    devs = mesh.shape["dev"]

    def per_device(pooled_grad, row_ids, scale_exps, table_owner, dense_acts, dense_cot):
        samples, tables, feat = pooled_grad.shape
        pool = row_ids.shape[1]
        owned = tables // devs
        hid, hid2 = dense_acts.shape[1], dense_cot.shape[1]
        tall, wide = hid // 2, hid2 // 2
        zs = devs // 4
        rows = owned * (samples + pool)
        total = tall * wide // 128
        half = total // 2
        dma = pltpu.SemaphoreType.DMA
        vmem = pl.BlockSpec(memory_space=pltpu.VMEM)
        hbm = pl.BlockSpec(memory_space=pltpu.HBM)
        f32, bf16, i32 = jnp.float32, jnp.bfloat16, jnp.int32
        buffers = [
            pltpu.VMEM((samples, tables, feat), bf16),
            pltpu.VMEM((tables, samples + PAD, feat), f32),
            pltpu.VMEM((pool, tables, samples), i32),
            pltpu.VMEM((tables, samples), i32),
            pltpu.VMEM((tables, 8, samples), f32),
            pltpu.VMEM((SPAN, 2 * samples), bf16),
            pltpu.VMEM((devs, rows, feat), bf16),
            pltpu.VMEM((2, devs, rows, feat), bf16),
            pltpu.VMEM((3, zs, rows, feat), bf16),
            pltpu.VMEM((4 * samples, tall), bf16),
            pltpu.VMEM((4 * samples, wide), bf16),
            pltpu.VMEM((samples, tall), bf16),
            pltpu.VMEM((samples, wide), bf16),
            pltpu.VMEM((total, 128), f32),
            pltpu.VMEM((half, 128), f32),
            pltpu.VMEM((zs, half // zs, 128), f32),
            pltpu.VMEM((3, 8, 128), f32),
            pltpu.VMEM((8, 128), f32),
            pltpu.VMEM((zs, 8, 128), f32),
            pltpu.VMEM((8, 128), f32),
        ]
        held = sum(math.prod(b.shape) * jnp.dtype(b.dtype).itemsize for b in buffers)
        partial = pl.pallas_call(
            functools.partial(kernel, devs, pool),
            out_shape=(
                jax.ShapeDtypeStruct((owned, ROWS, feat), f32),
                jax.ShapeDtypeStruct((4, total, 128), f32),
                jax.ShapeDtypeStruct((1, hid2), f32),
            ),
            in_specs=[hbm] * 6,
            out_specs=(vmem, vmem, vmem),
            scratch_shapes=buffers[:6]
            + [pltpu.SMEM((tables,), i32)] * 2
            + buffers[6:]
            + [
                dma((7 + CHUNKS,)),
                dma((3, zs)),
                dma((3, zs)),
                dma((4, zs)),
                dma((4, zs)),
                dma((devs,)),
                dma((devs,)),
                dma((6,)),
                dma((6,)),
                dma((2,)),
                dma((2,)),
                dma((zs,)),
                dma((zs,)),
                dma((zs + 1,)),
                dma((zs + 1,)),
                dma((zs,)),
                dma((zs,)),
                dma((7,)),
                dma((7,)),
            ],
            compiler_params=pltpu.CompilerParams(
                collective_id=0,
                has_side_effects=True,
                vmem_limit_bytes=min(held + VMEM_SPARE, VMEM_MOST),
            ),
        )(
            pltpu.with_memory_space_constraint(table_owner, pltpu.HBM),
            pltpu.with_memory_space_constraint(pooled_grad, pltpu.HBM),
            pltpu.with_memory_space_constraint(jnp.transpose(row_ids, (1, 2, 0)), pltpu.HBM),
            pltpu.with_memory_space_constraint(jnp.transpose(scale_exps, (1, 0)), pltpu.HBM),
            pltpu.with_memory_space_constraint(dense_acts, pltpu.HBM),
            pltpu.with_memory_space_constraint(dense_cot, pltpu.HBM),
        )
        cols = total // tall
        table_grad, weight_grad, bias_grad = pl.pallas_call(
            place_outputs,
            out_shape=(
                jax.ShapeDtypeStruct((owned, ROWS, feat), f32),
                jax.ShapeDtypeStruct((hid, hid2), f32),
                jax.ShapeDtypeStruct((1, hid2), f32),
            ),
            in_specs=[vmem] * 3,
            out_specs=(hbm, hbm, hbm),
            scratch_shapes=[dma((owned + 4 * cols + 1,))],
            compiler_params=pltpu.CompilerParams(vmem_limit_bytes=16 << 20),
        )(*partial)
        return table_grad, weight_grad, bias_grad.reshape(hid2)

    return jax.shard_map(
        per_device,
        mesh=mesh,
        in_specs=(
            P(("grp", "dev"), None, None),
            P(("grp", "dev"), None, None),
            P(("grp", "dev"), None),
            P(),
            P(("grp", "dev"), None),
            P(("grp", "dev"), None),
        ),
        out_specs=(P("dev", None, None), P(), P()),
        check_vma=False,
    )
```

```python
import functools
import math

import jax
import jax.numpy as jnp
from jax import lax
from jax.experimental import pallas as pl
from jax.experimental.pallas import tpu as pltpu
from jax.sharding import PartitionSpec as P

ROWS = 1024
SPAN = 128
MESH = pl.DeviceIdType.MESH
CHUNKS = 4
PAD = 8
GROUP = 16
LEVELS = 32767.0
TINY = 1e-30
VMEM_MOST = 67043328
VMEM_SPARE = 8 << 20


def encode(ids):
    level = jnp.zeros(ids.shape, jnp.int32)
    scale = jnp.ones(ids.shape, jnp.float32)
    for k in range(1, ROWS // SPAN):
        level = jnp.where(ids >= k * SPAN, k, level)
        scale = jnp.where(ids >= k * SPAN, float(1 << k), scale)
    return (ids - level * SPAN + SPAN).astype(jnp.float32) * scale


def powers(exps):
    return (
        1.0
        + (exps >= 1).astype(jnp.float32)
        + 2.0 * (exps >= 2).astype(jnp.float32)
        + 4.0 * (exps >= 3).astype(jnp.float32)
    )


def kernel(
    devs,
    pool,
    owner_hbm,
    x_hbm,
    ids_hbm,
    exps_hbm,
    acts_hbm,
    cot_hbm,
    table_ref,
    whole,
    bias_ref,
    xv,
    xs,
    idv,
    exv,
    codes,
    base,
    owner_ref,
    slots,
    send,
    recv,
    inter,
    ga,
    gc,
    oa,
    oc,
    part,
    yh,
    zbuf,
    bp,
    bh,
    bz,
    bx,
    coded,
    steps,
    lsem,
    psend,
    precv,
    csend,
    crecv,
    fsend,
    frecv,
    isend,
    irecv,
    ysend,
    yrecv,
    zsend,
    zrecv,
    bsend,
    brecv,
    gsend,
    grecv,
    esend,
    erecv,
):
    me = lax.axis_index("dev")
    grp = lax.axis_index("grp")
    other = 1 - grp
    samples, tables, feat = x_hbm.shape
    owned = table_ref.shape[0]
    id_rows = owned * pool
    zs = devs // 4
    core = lax.rem(me, 2)
    xbit = lax.rem(lax.div(me, 2), 2)
    z = lax.div(me, 4)
    place = lax.rem(me, 4)
    tall, wide = oa.shape[1], oc.shape[1]
    cols = wide // 128
    half = part.shape[0] // 2
    piece = half // zs
    pitch = samples + PAD

    def remote(src, dst, ssem, rsem, dev, group):
        return pltpu.make_async_remote_copy(
            src_ref=src,
            dst_ref=dst,
            send_sem=ssem,
            recv_sem=rsem,
            device_id={"grp": group, "dev": dev},
            device_id_type=MESH,
        )

    places = (
        place,
        place + 1 - 2 * core,
        place + 2 - 4 * xbit,
        place + 3 - 4 * xbit - 2 * core,
    )
    near = z * 4 + places[1]
    across = z * 4 + places[2]

    def columns(ref, part_index, width):
        return ref.at[:, pl.ds(pl.multiple_of(part_index * width, 128), width)]

    def slot_rows(ref, index):
        return ref.at[pl.ds(pl.multiple_of(index * samples, 8), samples)]

    owner_load = pltpu.make_async_copy(owner_hbm, owner_ref, lsem.at[6 + CHUNKS])
    owner_load.start()
    loads = [
        pltpu.make_async_copy(columns(acts_hbm, core, tall), slot_rows(ga, place), lsem.at[0]),
        pltpu.make_async_copy(columns(cot_hbm, xbit, wide), slot_rows(gc, place), lsem.at[1]),
        pltpu.make_async_copy(columns(acts_hbm, 1 - core, tall), oa, lsem.at[2]),
        pltpu.make_async_copy(columns(cot_hbm, 1 - xbit, wide), oc, lsem.at[3]),
        pltpu.make_async_copy(exps_hbm, exv, lsem.at[4]),
        pltpu.make_async_copy(ids_hbm, idv, lsem.at[5]),
    ]
    step = samples // CHUNKS
    for c in range(CHUNKS):
        span = pl.ds(c * step, step)
        loads.append(pltpu.make_async_copy(x_hbm.at[span], xv.at[span], lsem.at[6 + c]))
    for load in loads:
        load.start()

    barrier = pltpu.get_barrier_semaphore()

    def greet(dev, group):
        pl.semaphore_signal(
            barrier, inc=1, device_id={"grp": group, "dev": dev}, device_id_type=MESH
        )

    for m in range(1, 4):
        greet(z * 4 + places[m], grp)

    @pl.loop(1, zs)
    def _(k):
        greet(lax.rem(z + k, zs) * 4 + place, grp)

    greet(me, other)

    base[...] = (
        (lax.broadcasted_iota(jnp.int32, base.shape, 0) + SPAN)
        .astype(jnp.float32)
        .astype(jnp.bfloat16)
    )

    owner_load.wait()

    @pl.loop(0, tables)
    def _(k):
        slots[k] = lax.fori_loop(
            0,
            tables,
            lambda t, found: jnp.maximum(found, (owner_ref[t] == k).astype(jnp.int32) * t),
            jnp.int32(0),
            unroll=16,
        )

    pl.semaphore_wait(barrier, 3 + zs)

    def plane_copies(m, slot):
        acts = oa if m in (1, 3) else slot_rows(ga, place)
        cots = oc if m in (2, 3) else slot_rows(gc, place)
        who = z * 4 + places[m]
        return (
            remote(
                acts, slot_rows(ga, slot), isend.at[2 * m - 2], irecv.at[2 * m - 2], who, grp
            ),
            remote(
                cots, slot_rows(gc, slot), isend.at[2 * m - 1], irecv.at[2 * m - 1], who, grp
            ),
        )

    for load in loads[:4]:
        load.wait()
    for m in (2, 3, 1):
        for copy in plane_copies(m, place):
            copy.start()

    loads[4].wait()
    loads[5].wait()
    for p in range(pool):
        codes.reshape(tables * 8, samples)[pl.ds(p, tables, stride=8), :] = encode(idv[p])

    flat = xs.reshape(tables * pitch, feat)
    for c in range(CHUNKS):
        loads[6 + c].wait()

        @pl.loop(0, tables // GROUP)
        def _(g):
            some = pl.ds(pl.multiple_of(g * GROUP, GROUP), GROUP)
            factor = powers(exv[some, :])
            first = g * (GROUP * pitch)
            for k in range(c * step, (c + 1) * step):
                bound = jnp.broadcast_to(factor[:, k : k + 1], (GROUP, feat))
                value = xv[k, some, :].astype(jnp.float32)
                rows = pl.ds(first + k, GROUP, stride=pitch)
                flat[rows, :] = jnp.clip(value, -bound, bound)

    def build(target, dst):
        picked = []
        for s in range(owned):
            t = slots[dst * owned + s]
            target[pl.ds(s * samples, samples), :] = xs[t][:samples].astype(jnp.bfloat16)
            picked.append(codes[t][:pool])
        target[pl.ds(owned * samples, id_rows), :] = jnp.concatenate(picked, axis=0).astype(
            jnp.bfloat16
        )

    def each_near(act, first=1, last=zs):
        @pl.loop(first, last)
        def _(i):
            @pl.loop(0, 2)
            def _(j):
                peer = z + i * (1 - 2 * j)
                pl.when((peer >= 0) & (peer < zs))(functools.partial(act, peer))

    def close(act):
        each_near(act, 1, 2)

    def rest(act):
        each_near(act, 2, zs)

    def column_copy(m, peer):
        return remote(
            send.at[peer * 4 + places[m]],
            inter.at[m - 1, peer],
            psend.at[m - 1, peer],
            precv.at[m - 1, peer],
            z * 4 + places[m],
            grp,
        )

    def level_copy(m, back=False):
        who = z * 4 + places[m]
        return remote(
            send.at[who],
            recv.at[0, who if back else me],
            psend.at[m - 1, z],
            precv.at[m - 1, z],
            who,
            grp,
        )

    def line_copy(m, peer):
        origin = send.at[peer * 4 + place] if m == 0 else inter.at[m - 1, peer]
        return remote(
            origin,
            recv.at[0, z * 4 + places[m]],
            csend.at[m, peer],
            crecv.at[m, z],
            peer * 4 + place,
            grp,
        )

    def line_wait(m, peer):
        landing = recv.at[0, peer * 4 + places[m]]
        remote(
            landing, landing, csend.at[m, peer], crecv.at[m, peer], peer * 4 + place, grp
        ).wait_recv()

    def forward(src):
        return remote(
            recv.at[0, src], recv.at[1, src], fsend.at[src], frecv.at[src], me, other
        )

    def first_line(peer):
        dst = peer * 4 + place
        build(send.at[dst], dst)
        line_copy(0, peer).start()

    def column_start(m):
        def act(peer):
            dst = peer * 4 + places[m]
            build(send.at[dst], dst)
            column_copy(m, peer).start()

        each_near(act)

    def level_start(m):
        build(send.at[z * 4 + places[m]], z * 4 + places[m])
        level_copy(m).start()

    def column_pass(m, each):
        def act(peer):
            column_copy(m, peer).wait_recv()
            line_copy(m, peer).start()

        each(act)

    def level_pass(m):
        level_copy(m, True).wait_recv()
        forward(z * 4 + places[m]).start()

    def line_pass(m, each):
        def act(peer):
            line_wait(m, peer)
            forward(peer * 4 + places[m]).start()

        each(act)

    def plane_finish():
        for m in range(1, 4):
            for copy in plane_copies(m, places[m]):
                copy.wait_recv()
        bias = jnp.sum(gc[...].astype(jnp.float32), axis=0, keepdims=True)
        bp[0] = jnp.zeros(bp.shape[1:], jnp.float32)
        for j in range(cols):
            bp[0, j : j + 1, :] = bias[:, j * 128 : (j + 1) * 128]
        each = cols // 2
        for which in (other, grp):
            for j in range(each):
                block = which * each + j
                part[pl.ds(pl.multiple_of(block * tall, 8), tall), :] = lax.dot_general(
                    ga[...],
                    gc[:, pl.ds(pl.multiple_of(block * 128, 128), 128)],
                    (((0,), (0,)), ((), ())),
                    preferred_element_type=jnp.float32,
                )
            if which is other:
                y_start()

    def y_copies():
        away = part.at[pl.ds(pl.multiple_of(other * half, 8), half)]
        return (
            remote(away, yh, ysend.at[0], yrecv.at[0], me, other),
            remote(bp.at[0], bh, ysend.at[1], yrecv.at[1], me, other),
        )

    def y_start():
        for copy in y_copies():
            copy.start()

    def y_finish():
        for copy in y_copies():
            copy.wait_recv()
        keep = pl.ds(pl.multiple_of(grp * half, 8), half)
        part[keep, :] = part[keep, :] + yh[...]
        bp[1] = bp[0] + bh[...]

    def piece_of(peer):
        return pl.ds(pl.multiple_of(grp * half + peer * piece, 8), piece)

    def z_copy(k, back=False):
        peer = lax.rem(z + k, zs)
        dev = peer * 4 + place
        origin, landing = (z, peer) if back else (peer, z)
        return (
            remote(
                part.at[piece_of(origin)],
                zbuf.at[landing],
                zsend.at[peer],
                zrecv.at[landing],
                dev,
                grp,
            ),
            remote(bp.at[1], bz.at[landing], bsend.at[peer], brecv.at[landing], dev, grp),
        )

    def z_start():
        @pl.loop(1, zs)
        def _(k):
            for copy in z_copy(k):
                copy.start()

    def z_finish():
        zbuf[z] = part[piece_of(z), :]
        bz[z] = bp[1]

        @pl.loop(1, zs)
        def _(k):
            for copy in z_copy(k, True):
                copy.wait_recv()

        total = lax.fori_loop(1, zs, lambda i, run: run + zbuf[i], zbuf[0])
        total = total.reshape(piece // 8, 8, 128)
        top = jnp.maximum(jnp.max(jnp.abs(total), axis=0), TINY)
        code = jnp.round(total * (LEVELS / top)).astype(jnp.int32)
        coded[place, grp, z] = code.reshape(piece, 128).astype(jnp.int16)
        steps[place, grp, z] = top * (1.0 / LEVELS)
        bp[2] = lax.fori_loop(1, zs, lambda i, run: run + bz[i], bz[0])

    def zg_copy(k, back=False):
        peer = lax.rem(z + k, zs)
        dev = peer * 4 + place
        origin = peer if back else z
        return [
            remote(ref.at[place, grp, origin], ref.at[place, grp, origin], ss, rs, dev, grp)
            for ref, ss, rs in (
                (coded, gsend.at[0, peer], grecv.at[0, origin]),
                (steps, gsend.at[1, peer], grecv.at[1, origin]),
            )
        ]

    def bias_copy():
        return remote(bp.at[2], bx, bsend.at[zs], brecv.at[zs], across, grp)

    def zg_start():
        @pl.loop(1, zs)
        def _(k):
            for copy in zg_copy(k):
                copy.start()

        bias_copy().start()

    def zg_finish():
        @pl.loop(1, zs)
        def _(k):
            for copy in zg_copy(k, True):
                copy.wait_recv()

    halves = (grp, other)

    def gather_copy(k, back=False):
        if k == 0:
            tile, which, dev, group = place, other if back else grp, me, other
        elif k < 3:
            tile, which, dev, group = places[2] if back else place, halves[k - 1], across, grp
        elif k < 5:
            tile, which, dev, group = places[1] if back else place, halves[k - 3], near, grp
        else:
            tile = places[3] if back else places[2]
            which, dev, group = halves[k - 5], near, grp
        return [
            remote(
                ref.at[tile, which], ref.at[tile, which], esend.at[i, k], erecv.at[i, k], dev, group
            )
            for i, ref in enumerate((coded, steps))
        ]

    def gather_start(*ks):
        for k in ks:
            for copy in gather_copy(k):
                copy.start()

    def gather_wait(*ks):
        for k in ks:
            for copy in gather_copy(k, True):
                copy.wait_recv()

    def decode(tile, which):
        @pl.loop(0, zs)
        def _(i):
            code = coded[tile, which, i].astype(jnp.int32).astype(jnp.float32)
            value = code.reshape(piece // 8, 8, 128) * steps[tile, which, i]
            rows = pl.ds(pl.multiple_of(which * half + i * piece, 8), piece)
            whole[tile, rows, :] = value.reshape(piece, 128)

    def accumulate(side, first, second):
        marks = jnp.concatenate(
            [
                recv[side, c, pl.ds(owned * samples, id_rows), :].astype(jnp.float32)
                for c in (first, second)
            ],
            axis=1,
        )
        one, zero = jnp.bfloat16(1), jnp.bfloat16(0)
        axis = base[...]
        for s in range(owned):
            values = jnp.concatenate(
                [recv[side, c, pl.ds(s * samples, samples), :] for c in (first, second)],
                axis=0,
            )
            rows = marks[s * pool : (s + 1) * pool]
            for block in range(ROWS // SPAN):
                local = (rows * (1.0 / (1 << block))).astype(jnp.bfloat16)
                counts = jnp.where(local[0:1] == axis, one, zero)
                for p in range(1, pool):
                    counts = counts + jnp.where(local[p : p + 1] == axis, one, zero)
                span = pl.ds(block * SPAN, SPAN)
                table_ref[s, span, :] = table_ref[s, span, :] + jnp.dot(
                    counts, values, preferred_element_type=jnp.float32
                )

    def pair(side, part_of, peer):
        accumulate(side, peer * 4 + places[2 * part_of], peer * 4 + places[2 * part_of + 1])

    def far_pair(part_of, peer):
        for m in (2 * part_of, 2 * part_of + 1):
            forward(peer * 4 + places[m]).wait_recv()
        pair(1, part_of, peer)

    each_near(first_line)
    build(recv.at[0, me], me)
    forward(me).start()
    level_start(1)
    level_start(2)
    level_start(3)
    column_start(1)
    column_start(2)
    column_start(3)
    column_pass(1, close)
    column_pass(1, rest)
    level_pass(1)
    table_ref[...] = jnp.zeros(table_ref.shape, jnp.float32)
    plane_finish()
    line_pass(0, close)
    y_finish()
    z_start()
    level_pass(2)
    level_pass(3)
    line_pass(0, rest)
    column_pass(2, close)
    pair(0, 0, z)
    line_pass(1, close)
    z_finish()
    zg_start()
    column_pass(2, rest)
    line_pass(1, rest)
    column_pass(3, close)
    column_pass(3, rest)
    close(functools.partial(pair, 0, 0))
    rest(functools.partial(pair, 0, 0))
    far_pair(0, z)
    line_pass(2, close)
    zg_finish()
    gather_start(0, 1, 3)
    line_pass(2, rest)
    pair(0, 1, z)
    close(functools.partial(far_pair, 0))
    rest(functools.partial(far_pair, 0))
    gather_wait(0)
    gather_start(2, 4)
    decode(place, grp)
    decode(place, other)
    line_pass(3, close)
    line_pass(3, rest)
    close(functools.partial(pair, 0, 1))
    rest(functools.partial(pair, 0, 1))
    gather_wait(1)
    gather_start(5)
    decode(places[2], grp)
    far_pair(1, z)
    gather_wait(2)
    gather_start(6)
    decode(places[2], other)
    close(functools.partial(far_pair, 1))
    rest(functools.partial(far_pair, 1))
    gather_wait(3, 4)
    decode(places[1], grp)
    decode(places[1], other)
    gather_wait(5, 6)
    decode(places[3], grp)
    decode(places[3], other)

    bias_copy().wait_recv()
    mine, theirs = bp[2], bx[...]
    lower = jnp.where(xbit == 0, mine, theirs)
    upper = jnp.where(xbit == 0, theirs, mine)
    for j in range(cols):
        bias_ref[:, j * 128 : (j + 1) * 128] = lower[j : j + 1, :]
        bias_ref[:, (cols + j) * 128 : (cols + j + 1) * 128] = upper[j : j + 1, :]

    bias_copy().wait_send()
    for copy in y_copies():
        copy.wait_send()
    for k in range(7):
        for copy in gather_copy(k):
            copy.wait_send()
    for m in range(1, 4):
        level_copy(m).wait_send()
        for copy in plane_copies(m, place):
            copy.wait_send()

    @pl.loop(1, zs)
    def _(k):
        for copy in z_copy(k):
            copy.wait_send()
        for copy in zg_copy(k):
            copy.wait_send()

    def drain(peer):
        for m in range(4):
            line_copy(m, peer).wait_send()
            if m > 0:
                column_copy(m, peer).wait_send()

    each_near(drain)

    @pl.loop(0, devs)
    def _(src):
        forward(src).wait_send()


def place_outputs(table_in, whole_in, bias_in, table_out, weight_out, bias_out, sems):
    tiles, rows, _ = whole_in.shape
    tall = weight_out.shape[0] // 2
    cols = rows // tall
    copies = []
    for s in range(table_in.shape[0]):
        copies.append((table_in.at[s], table_out.at[s]))
    for tile in range(tiles):
        for j in range(cols):
            block = (tile // 2) * cols + j
            copies.append(
                (
                    whole_in.at[tile, pl.ds(j * tall, tall)],
                    weight_out.at[pl.ds((tile % 2) * tall, tall), pl.ds(block * 128, 128)],
                )
            )
    copies.append((bias_in, bias_out))
    started = [
        pltpu.make_async_copy(src, dst, sems.at[i]) for i, (src, dst) in enumerate(copies)
    ]
    for copy in started:
        copy.start()
    for copy in started:
        copy.wait()


def solution(mesh):
    devs = mesh.shape["dev"]

    def per_device(pooled_grad, row_ids, scale_exps, table_owner, dense_acts, dense_cot):
        samples, tables, feat = pooled_grad.shape
        pool = row_ids.shape[1]
        owned = tables // devs
        hid, hid2 = dense_acts.shape[1], dense_cot.shape[1]
        tall, wide = hid // 2, hid2 // 2
        zs = devs // 4
        rows = owned * (samples + pool)
        total = tall * wide // 128
        half = total // 2
        dma = pltpu.SemaphoreType.DMA
        vmem = pl.BlockSpec(memory_space=pltpu.VMEM)
        hbm = pl.BlockSpec(memory_space=pltpu.HBM)
        f32, bf16, i32 = jnp.float32, jnp.bfloat16, jnp.int32
        buffers = [
            pltpu.VMEM((samples, tables, feat), bf16),
            pltpu.VMEM((tables, samples + PAD, feat), f32),
            pltpu.VMEM((pool, tables, samples), i32),
            pltpu.VMEM((tables, samples), i32),
            pltpu.VMEM((tables, 8, samples), f32),
            pltpu.VMEM((SPAN, 2 * samples), bf16),
            pltpu.VMEM((devs, rows, feat), bf16),
            pltpu.VMEM((2, devs, rows, feat), bf16),
            pltpu.VMEM((3, zs, rows, feat), bf16),
            pltpu.VMEM((4 * samples, tall), bf16),
            pltpu.VMEM((4 * samples, wide), bf16),
            pltpu.VMEM((samples, tall), bf16),
            pltpu.VMEM((samples, wide), bf16),
            pltpu.VMEM((total, 128), f32),
            pltpu.VMEM((half, 128), f32),
            pltpu.VMEM((zs, half // zs, 128), f32),
            pltpu.VMEM((3, 8, 128), f32),
            pltpu.VMEM((8, 128), f32),
            pltpu.VMEM((zs, 8, 128), f32),
            pltpu.VMEM((8, 128), f32),
            pltpu.VMEM((4, 2, zs, half // zs, 128), jnp.int16),
            pltpu.VMEM((4, 2, zs, 8, 128), f32),
        ]
        held = sum(math.prod(b.shape) * jnp.dtype(b.dtype).itemsize for b in buffers)
        partial = pl.pallas_call(
            functools.partial(kernel, devs, pool),
            out_shape=(
                jax.ShapeDtypeStruct((owned, ROWS, feat), f32),
                jax.ShapeDtypeStruct((4, total, 128), f32),
                jax.ShapeDtypeStruct((1, hid2), f32),
            ),
            in_specs=[hbm] * 6,
            out_specs=(vmem, vmem, vmem),
            scratch_shapes=buffers[:6]
            + [pltpu.SMEM((tables,), i32)] * 2
            + buffers[6:]
            + [
                dma((7 + CHUNKS,)),
                dma((3, zs)),
                dma((3, zs)),
                dma((4, zs)),
                dma((4, zs)),
                dma((devs,)),
                dma((devs,)),
                dma((6,)),
                dma((6,)),
                dma((2,)),
                dma((2,)),
                dma((zs,)),
                dma((zs,)),
                dma((zs + 1,)),
                dma((zs + 1,)),
                dma((2, zs)),
                dma((2, zs)),
                dma((2, 7)),
                dma((2, 7)),
            ],
            compiler_params=pltpu.CompilerParams(
                collective_id=0,
                has_side_effects=True,
                vmem_limit_bytes=min(held + VMEM_SPARE, VMEM_MOST),
            ),
        )(
            pltpu.with_memory_space_constraint(table_owner, pltpu.HBM),
            pltpu.with_memory_space_constraint(pooled_grad, pltpu.HBM),
            pltpu.with_memory_space_constraint(jnp.transpose(row_ids, (1, 2, 0)), pltpu.HBM),
            pltpu.with_memory_space_constraint(jnp.transpose(scale_exps, (1, 0)), pltpu.HBM),
            pltpu.with_memory_space_constraint(dense_acts, pltpu.HBM),
            pltpu.with_memory_space_constraint(dense_cot, pltpu.HBM),
        )
        cols = total // tall
        table_grad, weight_grad, bias_grad = pl.pallas_call(
            place_outputs,
            out_shape=(
                jax.ShapeDtypeStruct((owned, ROWS, feat), f32),
                jax.ShapeDtypeStruct((hid, hid2), f32),
                jax.ShapeDtypeStruct((1, hid2), f32),
            ),
            in_specs=[vmem] * 3,
            out_specs=(hbm, hbm, hbm),
            scratch_shapes=[dma((owned + 4 * cols + 1,))],
            compiler_params=pltpu.CompilerParams(vmem_limit_bytes=16 << 20),
        )(*partial)
        return table_grad, weight_grad, bias_grad.reshape(hid2)

    return jax.shard_map(
        per_device,
        mesh=mesh,
        in_specs=(
            P(("grp", "dev"), None, None),
            P(("grp", "dev"), None, None),
            P(("grp", "dev"), None),
            P(),
            P(("grp", "dev"), None),
            P(("grp", "dev"), None),
        ),
        out_specs=(P("dev", None, None), P(), P()),
        check_vma=False,
    )
```

```python
import functools
import math

import jax
import jax.numpy as jnp
from jax import lax
from jax.experimental import pallas as pl
from jax.experimental.pallas import tpu as pltpu
from jax.sharding import PartitionSpec as P

ROWS = 1024
SPAN = 128
MESH = pl.DeviceIdType.MESH
CHUNKS = 1
PAD = 8
GROUP = 16
LEVELS = 32767.0
TINY = 1e-30
VMEM_MOST = 67043328
VMEM_SPARE = 8 << 20


def encode(ids):
    level = jnp.zeros(ids.shape, jnp.int32)
    scale = jnp.ones(ids.shape, jnp.float32)
    for k in range(1, ROWS // SPAN):
        level = jnp.where(ids >= k * SPAN, k, level)
        scale = jnp.where(ids >= k * SPAN, float(1 << k), scale)
    return (ids - level * SPAN + SPAN).astype(jnp.float32) * scale


def powers(exps):
    return (
        1.0
        + (exps >= 1).astype(jnp.float32)
        + 2.0 * (exps >= 2).astype(jnp.float32)
        + 4.0 * (exps >= 3).astype(jnp.float32)
    )


def kernel(
    devs,
    pool,
    owner_hbm,
    x_hbm,
    ids_hbm,
    exps_hbm,
    acts_hbm,
    cot_hbm,
    table_ref,
    whole,
    bias_ref,
    xv,
    xs,
    idv,
    exv,
    codes,
    base,
    owner_ref,
    slots,
    send,
    recv,
    inter,
    ga,
    gc,
    oa,
    oc,
    part,
    yh,
    zbuf,
    bp,
    bh,
    bz,
    bx,
    coded,
    steps,
    lsem,
    psend,
    precv,
    csend,
    crecv,
    fsend,
    frecv,
    isend,
    irecv,
    ysend,
    yrecv,
    zsend,
    zrecv,
    bsend,
    brecv,
    gsend,
    grecv,
    esend,
    erecv,
):
    me = lax.axis_index("dev")
    grp = lax.axis_index("grp")
    other = 1 - grp
    samples, tables, feat = x_hbm.shape
    owned = table_ref.shape[0]
    id_rows = owned * pool
    zs = devs // 4
    core = lax.rem(me, 2)
    xbit = lax.rem(lax.div(me, 2), 2)
    z = lax.div(me, 4)
    place = lax.rem(me, 4)
    tall, wide = oa.shape[1], oc.shape[1]
    cols = wide // 128
    half = part.shape[0] // 2
    piece = half // zs
    pitch = samples + PAD

    def remote(src, dst, ssem, rsem, dev, group):
        return pltpu.make_async_remote_copy(
            src_ref=src,
            dst_ref=dst,
            send_sem=ssem,
            recv_sem=rsem,
            device_id={"grp": group, "dev": dev},
            device_id_type=MESH,
        )

    places = (
        place,
        place + 1 - 2 * core,
        place + 2 - 4 * xbit,
        place + 3 - 4 * xbit - 2 * core,
    )
    near = z * 4 + places[1]
    across = z * 4 + places[2]

    def columns(ref, part_index, width):
        return ref.at[:, pl.ds(pl.multiple_of(part_index * width, 128), width)]

    def slot_rows(ref, index):
        return ref.at[pl.ds(pl.multiple_of(index * samples, 8), samples)]

    owner_load = pltpu.make_async_copy(owner_hbm, owner_ref, lsem.at[6 + CHUNKS])
    owner_load.start()
    loads = [
        pltpu.make_async_copy(columns(acts_hbm, core, tall), slot_rows(ga, place), lsem.at[0]),
        pltpu.make_async_copy(columns(cot_hbm, xbit, wide), slot_rows(gc, place), lsem.at[1]),
        pltpu.make_async_copy(columns(acts_hbm, 1 - core, tall), oa, lsem.at[2]),
        pltpu.make_async_copy(columns(cot_hbm, 1 - xbit, wide), oc, lsem.at[3]),
        pltpu.make_async_copy(exps_hbm, exv, lsem.at[4]),
        pltpu.make_async_copy(ids_hbm, idv, lsem.at[5]),
    ]
    step = samples // CHUNKS
    for c in range(CHUNKS):
        span = pl.ds(c * step, step)
        loads.append(pltpu.make_async_copy(x_hbm.at[span], xv.at[span], lsem.at[6 + c]))
    for load in loads:
        load.start()

    barrier = pltpu.get_barrier_semaphore()

    def greet(dev, group):
        pl.semaphore_signal(
            barrier, inc=1, device_id={"grp": group, "dev": dev}, device_id_type=MESH
        )

    for m in range(1, 4):
        greet(z * 4 + places[m], grp)

    @pl.loop(1, zs)
    def _(k):
        greet(lax.rem(z + k, zs) * 4 + place, grp)

    greet(me, other)

    base[...] = (
        (lax.broadcasted_iota(jnp.int32, base.shape, 0) + SPAN)
        .astype(jnp.float32)
        .astype(jnp.bfloat16)
    )

    owner_load.wait()

    @pl.loop(0, tables)
    def _(k):
        slots[k] = lax.fori_loop(
            0,
            tables,
            lambda t, found: jnp.maximum(found, (owner_ref[t] == k).astype(jnp.int32) * t),
            jnp.int32(0),
            unroll=16,
        )

    pl.semaphore_wait(barrier, 3 + zs)

    def plane_copies(m, slot):
        acts = oa if m in (1, 3) else slot_rows(ga, place)
        cots = oc if m in (2, 3) else slot_rows(gc, place)
        who = z * 4 + places[m]
        return (
            remote(
                acts, slot_rows(ga, slot), isend.at[2 * m - 2], irecv.at[2 * m - 2], who, grp
            ),
            remote(
                cots, slot_rows(gc, slot), isend.at[2 * m - 1], irecv.at[2 * m - 1], who, grp
            ),
        )

    for load in loads[:4]:
        load.wait()
    for m in (2, 3, 1):
        for copy in plane_copies(m, place):
            copy.start()

    loads[4].wait()
    loads[5].wait()
    for p in range(pool):
        codes.reshape(tables * 8, samples)[pl.ds(p, tables, stride=8), :] = encode(idv[p])

    flat = xs.reshape(tables * pitch, feat)
    for c in range(CHUNKS):
        loads[6 + c].wait()

        @pl.loop(0, tables // GROUP)
        def _(g):
            some = pl.ds(pl.multiple_of(g * GROUP, GROUP), GROUP)
            factor = powers(exv[some, :])
            first = g * (GROUP * pitch)
            for k in range(c * step, (c + 1) * step):
                bound = jnp.broadcast_to(factor[:, k : k + 1], (GROUP, feat))
                value = xv[k, some, :].astype(jnp.float32)
                rows = pl.ds(first + k, GROUP, stride=pitch)
                flat[rows, :] = jnp.clip(value, -bound, bound)

    def build(target, dst):
        picked = []
        for s in range(owned):
            t = slots[dst * owned + s]
            target[pl.ds(s * samples, samples), :] = xs[t][:samples].astype(jnp.bfloat16)
            picked.append(codes[t][:pool])
        target[pl.ds(owned * samples, id_rows), :] = jnp.concatenate(picked, axis=0).astype(
            jnp.bfloat16
        )

    def each_near(act, first=1, last=zs):
        @pl.loop(first, last)
        def _(i):
            @pl.loop(0, 2)
            def _(j):
                peer = z + i * (1 - 2 * j)
                pl.when((peer >= 0) & (peer < zs))(functools.partial(act, peer))

    def close(act):
        each_near(act, 1, 2)

    def rest(act):
        each_near(act, 2, zs)

    def column_copy(m, peer):
        return remote(
            send.at[peer * 4 + places[m]],
            inter.at[m - 1, peer],
            psend.at[m - 1, peer],
            precv.at[m - 1, peer],
            z * 4 + places[m],
            grp,
        )

    def level_copy(m, back=False):
        who = z * 4 + places[m]
        return remote(
            send.at[who],
            recv.at[0, who if back else me],
            psend.at[m - 1, z],
            precv.at[m - 1, z],
            who,
            grp,
        )

    def line_copy(m, peer):
        origin = send.at[peer * 4 + place] if m == 0 else inter.at[m - 1, peer]
        return remote(
            origin,
            recv.at[0, z * 4 + places[m]],
            csend.at[m, peer],
            crecv.at[m, z],
            peer * 4 + place,
            grp,
        )

    def line_wait(m, peer):
        landing = recv.at[0, peer * 4 + places[m]]
        remote(
            landing, landing, csend.at[m, peer], crecv.at[m, peer], peer * 4 + place, grp
        ).wait_recv()

    def forward(src):
        return remote(
            recv.at[0, src], recv.at[1, src], fsend.at[src], frecv.at[src], me, other
        )

    def first_line(peer):
        dst = peer * 4 + place
        build(send.at[dst], dst)
        line_copy(0, peer).start()

    def column_start(m):
        def act(peer):
            dst = peer * 4 + places[m]
            build(send.at[dst], dst)
            column_copy(m, peer).start()

        each_near(act)

    def level_start(m):
        build(send.at[z * 4 + places[m]], z * 4 + places[m])
        level_copy(m).start()

    def column_pass(m, each):
        def act(peer):
            column_copy(m, peer).wait_recv()
            line_copy(m, peer).start()

        each(act)

    def level_pass(m):
        level_copy(m, True).wait_recv()
        forward(z * 4 + places[m]).start()

    def line_pass(m, each):
        def act(peer):
            line_wait(m, peer)
            forward(peer * 4 + places[m]).start()

        each(act)

    def plane_finish():
        for m in range(1, 4):
            for copy in plane_copies(m, places[m]):
                copy.wait_recv()
        bias = jnp.sum(gc[...].astype(jnp.float32), axis=0, keepdims=True)
        bp[0] = jnp.zeros(bp.shape[1:], jnp.float32)
        for j in range(cols):
            bp[0, j : j + 1, :] = bias[:, j * 128 : (j + 1) * 128]
        each = cols // 2
        for which in (other, grp):
            for j in range(each):
                block = which * each + j
                part[pl.ds(pl.multiple_of(block * tall, 8), tall), :] = lax.dot_general(
                    ga[...],
                    gc[:, pl.ds(pl.multiple_of(block * 128, 128), 128)],
                    (((0,), (0,)), ((), ())),
                    preferred_element_type=jnp.float32,
                )
            if which is other:
                y_start()

    def y_copies():
        away = part.at[pl.ds(pl.multiple_of(other * half, 8), half)]
        return (
            remote(away, yh, ysend.at[0], yrecv.at[0], me, other),
            remote(bp.at[0], bh, ysend.at[1], yrecv.at[1], me, other),
        )

    def y_start():
        for copy in y_copies():
            copy.start()

    def y_finish():
        for copy in y_copies():
            copy.wait_recv()
        keep = pl.ds(pl.multiple_of(grp * half, 8), half)
        part[keep, :] = part[keep, :] + yh[...]
        bp[1] = bp[0] + bh[...]

    def piece_of(peer):
        return pl.ds(pl.multiple_of(grp * half + peer * piece, 8), piece)

    def z_copy(k, back=False):
        peer = lax.rem(z + k, zs)
        dev = peer * 4 + place
        origin, landing = (z, peer) if back else (peer, z)
        return (
            remote(
                part.at[piece_of(origin)],
                zbuf.at[landing],
                zsend.at[peer],
                zrecv.at[landing],
                dev,
                grp,
            ),
            remote(bp.at[1], bz.at[landing], bsend.at[peer], brecv.at[landing], dev, grp),
        )

    def z_start():
        @pl.loop(1, zs)
        def _(k):
            for copy in z_copy(k):
                copy.start()

    def z_finish():
        zbuf[z] = part[piece_of(z), :]
        bz[z] = bp[1]

        @pl.loop(1, zs)
        def _(k):
            for copy in z_copy(k, True):
                copy.wait_recv()

        total = lax.fori_loop(1, zs, lambda i, run: run + zbuf[i], zbuf[0])
        top = jnp.maximum(jnp.max(jnp.abs(total), axis=0, keepdims=True), TINY)
        coded[place, grp, z] = jnp.round(total * (LEVELS / top)).astype(jnp.int32).astype(jnp.int16)
        steps[place, grp, z] = top * (1.0 / LEVELS)
        bp[2] = lax.fori_loop(1, zs, lambda i, run: run + bz[i], bz[0])

    def zg_copy(k, back=False):
        peer = lax.rem(z + k, zs)
        dev = peer * 4 + place
        origin = peer if back else z
        return [
            remote(ref.at[place, grp, origin], ref.at[place, grp, origin], ss, rs, dev, grp)
            for ref, ss, rs in (
                (coded, gsend.at[0, peer], grecv.at[0, origin]),
                (steps, gsend.at[1, peer], grecv.at[1, origin]),
            )
        ]

    def bias_copy():
        return remote(bp.at[2], bx, bsend.at[zs], brecv.at[zs], across, grp)

    def zg_start():
        @pl.loop(1, zs)
        def _(k):
            for copy in zg_copy(k):
                copy.start()

        bias_copy().start()

    def zg_finish():
        @pl.loop(1, zs)
        def _(k):
            for copy in zg_copy(k, True):
                copy.wait_recv()

    halves = (grp, other)

    def gather_copy(k, back=False):
        if k == 0:
            tile, which, dev, group = place, other if back else grp, me, other
        elif k < 3:
            tile, which, dev, group = places[2] if back else place, halves[k - 1], across, grp
        elif k < 5:
            tile, which, dev, group = places[1] if back else place, halves[k - 3], near, grp
        else:
            tile = places[3] if back else places[2]
            which, dev, group = halves[k - 5], near, grp
        return [
            remote(
                ref.at[tile, which], ref.at[tile, which], esend.at[i, k], erecv.at[i, k], dev, group
            )
            for i, ref in enumerate((coded, steps))
        ]

    def gather_start(*ks):
        for k in ks:
            for copy in gather_copy(k):
                copy.start()

    def gather_wait(*ks):
        for k in ks:
            for copy in gather_copy(k, True):
                copy.wait_recv()

    def decode(tile, which):
        @pl.loop(0, zs)
        def _(i):
            code = coded[tile, which, i].astype(jnp.int32).astype(jnp.float32)
            rows = pl.ds(pl.multiple_of(which * half + i * piece, 8), piece)
            whole[tile, rows, :] = code * steps[tile, which, i]

    def accumulate(side, first, second):
        marks = jnp.concatenate(
            [
                recv[side, c, pl.ds(owned * samples, id_rows), :].astype(jnp.float32)
                for c in (first, second)
            ],
            axis=1,
        )
        one, zero = jnp.bfloat16(1), jnp.bfloat16(0)
        axis = base[...]
        for s in range(owned):
            values = jnp.concatenate(
                [recv[side, c, pl.ds(s * samples, samples), :] for c in (first, second)],
                axis=0,
            )
            rows = marks[s * pool : (s + 1) * pool]
            for block in range(ROWS // SPAN):
                local = (rows * (1.0 / (1 << block))).astype(jnp.bfloat16)
                counts = jnp.where(local[0:1] == axis, one, zero)
                for p in range(1, pool):
                    counts = counts + jnp.where(local[p : p + 1] == axis, one, zero)
                span = pl.ds(block * SPAN, SPAN)
                table_ref[s, span, :] = table_ref[s, span, :] + jnp.dot(
                    counts, values, preferred_element_type=jnp.float32
                )

    def pair(side, part_of, peer):
        accumulate(side, peer * 4 + places[2 * part_of], peer * 4 + places[2 * part_of + 1])

    def far_pair(part_of, peer):
        for m in (2 * part_of, 2 * part_of + 1):
            forward(peer * 4 + places[m]).wait_recv()
        pair(1, part_of, peer)

    each_near(first_line)
    build(recv.at[0, me], me)
    forward(me).start()
    level_start(1)
    column_start(2)
    level_start(2)
    level_start(3)
    column_start(1)
    column_start(3)
    column_pass(1, close)
    plane_finish()
    column_pass(1, rest)
    level_pass(1)
    table_ref[...] = jnp.zeros(table_ref.shape, jnp.float32)
    line_pass(0, close)
    y_finish()
    z_start()
    level_pass(2)
    level_pass(3)
    line_pass(0, rest)
    column_pass(2, close)
    pair(0, 0, z)
    line_pass(1, close)
    z_finish()
    zg_start()
    column_pass(2, rest)
    line_pass(1, rest)
    zg_finish()
    gather_start(0, 1, 3)
    column_pass(3, close)
    column_pass(3, rest)
    close(functools.partial(pair, 0, 0))
    rest(functools.partial(pair, 0, 0))
    far_pair(0, z)
    line_pass(2, close)
    line_pass(2, rest)
    pair(0, 1, z)
    close(functools.partial(far_pair, 0))
    rest(functools.partial(far_pair, 0))
    gather_wait(0)
    gather_start(2, 4)
    decode(place, grp)
    decode(place, other)
    line_pass(3, close)
    line_pass(3, rest)
    close(functools.partial(pair, 0, 1))
    rest(functools.partial(pair, 0, 1))
    gather_wait(1)
    gather_start(5)
    decode(places[2], grp)
    far_pair(1, z)
    gather_wait(2)
    gather_start(6)
    decode(places[2], other)
    close(functools.partial(far_pair, 1))
    rest(functools.partial(far_pair, 1))
    gather_wait(3, 4)
    decode(places[1], grp)
    decode(places[1], other)
    gather_wait(5, 6)
    decode(places[3], grp)
    decode(places[3], other)

    bias_copy().wait_recv()
    mine, theirs = bp[2], bx[...]
    lower = jnp.where(xbit == 0, mine, theirs)
    upper = jnp.where(xbit == 0, theirs, mine)
    for j in range(cols):
        bias_ref[:, j * 128 : (j + 1) * 128] = lower[j : j + 1, :]
        bias_ref[:, (cols + j) * 128 : (cols + j + 1) * 128] = upper[j : j + 1, :]

    bias_copy().wait_send()
    for copy in y_copies():
        copy.wait_send()
    for k in range(7):
        for copy in gather_copy(k):
            copy.wait_send()
    for m in range(1, 4):
        level_copy(m).wait_send()
        for copy in plane_copies(m, place):
            copy.wait_send()

    @pl.loop(1, zs)
    def _(k):
        for copy in z_copy(k):
            copy.wait_send()
        for copy in zg_copy(k):
            copy.wait_send()

    def drain(peer):
        for m in range(4):
            line_copy(m, peer).wait_send()
            if m > 0:
                column_copy(m, peer).wait_send()

    each_near(drain)

    @pl.loop(0, devs)
    def _(src):
        forward(src).wait_send()


def place_outputs(table_in, whole_in, bias_in, table_out, weight_out, bias_out, sems):
    tiles, rows, _ = whole_in.shape
    tall = weight_out.shape[0] // 2
    cols = rows // tall
    copies = []
    for s in range(table_in.shape[0]):
        copies.append((table_in.at[s], table_out.at[s]))
    for tile in range(tiles):
        for j in range(cols):
            block = (tile // 2) * cols + j
            copies.append(
                (
                    whole_in.at[tile, pl.ds(j * tall, tall)],
                    weight_out.at[pl.ds((tile % 2) * tall, tall), pl.ds(block * 128, 128)],
                )
            )
    copies.append((bias_in, bias_out))
    started = [
        pltpu.make_async_copy(src, dst, sems.at[i]) for i, (src, dst) in enumerate(copies)
    ]
    for copy in started:
        copy.start()
    for copy in started:
        copy.wait()


def solution(mesh):
    devs = mesh.shape["dev"]

    def per_device(pooled_grad, row_ids, scale_exps, table_owner, dense_acts, dense_cot):
        samples, tables, feat = pooled_grad.shape
        pool = row_ids.shape[1]
        owned = tables // devs
        hid, hid2 = dense_acts.shape[1], dense_cot.shape[1]
        tall, wide = hid // 2, hid2 // 2
        zs = devs // 4
        rows = owned * (samples + pool)
        total = tall * wide // 128
        half = total // 2
        dma = pltpu.SemaphoreType.DMA
        vmem = pl.BlockSpec(memory_space=pltpu.VMEM)
        hbm = pl.BlockSpec(memory_space=pltpu.HBM)
        f32, bf16, i32 = jnp.float32, jnp.bfloat16, jnp.int32
        buffers = [
            pltpu.VMEM((samples, tables, feat), bf16),
            pltpu.VMEM((tables, samples + PAD, feat), f32),
            pltpu.VMEM((pool, tables, samples), i32),
            pltpu.VMEM((tables, samples), i32),
            pltpu.VMEM((tables, 8, samples), f32),
            pltpu.VMEM((SPAN, 2 * samples), bf16),
            pltpu.VMEM((devs, rows, feat), bf16),
            pltpu.VMEM((2, devs, rows, feat), bf16),
            pltpu.VMEM((3, zs, rows, feat), bf16),
            pltpu.VMEM((4 * samples, tall), bf16),
            pltpu.VMEM((4 * samples, wide), bf16),
            pltpu.VMEM((samples, tall), bf16),
            pltpu.VMEM((samples, wide), bf16),
            pltpu.VMEM((total, 128), f32),
            pltpu.VMEM((half, 128), f32),
            pltpu.VMEM((zs, half // zs, 128), f32),
            pltpu.VMEM((3, 8, 128), f32),
            pltpu.VMEM((8, 128), f32),
            pltpu.VMEM((zs, 8, 128), f32),
            pltpu.VMEM((8, 128), f32),
            pltpu.VMEM((4, 2, zs, half // zs, 128), jnp.int16),
            pltpu.VMEM((4, 2, zs, 1, 128), f32),
        ]
        held = sum(math.prod(b.shape) * jnp.dtype(b.dtype).itemsize for b in buffers)
        partial = pl.pallas_call(
            functools.partial(kernel, devs, pool),
            out_shape=(
                jax.ShapeDtypeStruct((owned, ROWS, feat), f32),
                jax.ShapeDtypeStruct((4, total, 128), f32),
                jax.ShapeDtypeStruct((1, hid2), f32),
            ),
            in_specs=[hbm] * 6,
            out_specs=(vmem, vmem, vmem),
            scratch_shapes=buffers[:6]
            + [pltpu.SMEM((tables,), i32)] * 2
            + buffers[6:]
            + [
                dma((7 + CHUNKS,)),
                dma((3, zs)),
                dma((3, zs)),
                dma((4, zs)),
                dma((4, zs)),
                dma((devs,)),
                dma((devs,)),
                dma((6,)),
                dma((6,)),
                dma((2,)),
                dma((2,)),
                dma((zs,)),
                dma((zs,)),
                dma((zs + 1,)),
                dma((zs + 1,)),
                dma((2, zs)),
                dma((2, zs)),
                dma((2, 7)),
                dma((2, 7)),
            ],
            compiler_params=pltpu.CompilerParams(
                collective_id=0,
                has_side_effects=True,
                vmem_limit_bytes=min(held + VMEM_SPARE, VMEM_MOST),
            ),
        )(
            pltpu.with_memory_space_constraint(table_owner, pltpu.HBM),
            pltpu.with_memory_space_constraint(pooled_grad, pltpu.HBM),
            pltpu.with_memory_space_constraint(jnp.transpose(row_ids, (1, 2, 0)), pltpu.HBM),
            pltpu.with_memory_space_constraint(jnp.transpose(scale_exps, (1, 0)), pltpu.HBM),
            pltpu.with_memory_space_constraint(dense_acts, pltpu.HBM),
            pltpu.with_memory_space_constraint(dense_cot, pltpu.HBM),
        )
        cols = total // tall
        table_grad, weight_grad, bias_grad = pl.pallas_call(
            place_outputs,
            out_shape=(
                jax.ShapeDtypeStruct((owned, ROWS, feat), f32),
                jax.ShapeDtypeStruct((hid, hid2), f32),
                jax.ShapeDtypeStruct((1, hid2), f32),
            ),
            in_specs=[vmem] * 3,
            out_specs=(hbm, hbm, hbm),
            scratch_shapes=[dma((owned + 4 * cols + 1,))],
            compiler_params=pltpu.CompilerParams(vmem_limit_bytes=16 << 20),
        )(*partial)
        return table_grad, weight_grad, bias_grad.reshape(hid2)

    return jax.shard_map(
        per_device,
        mesh=mesh,
        in_specs=(
            P(("grp", "dev"), None, None),
            P(("grp", "dev"), None, None),
            P(("grp", "dev"), None),
            P(),
            P(("grp", "dev"), None),
            P(("grp", "dev"), None),
        ),
        out_specs=(P("dev", None, None), P(), P()),
        check_vma=False,
    )
```

```python
import functools
import math

import jax
import jax.numpy as jnp
from jax import lax
from jax.experimental import pallas as pl
from jax.experimental.pallas import tpu as pltpu
from jax.sharding import PartitionSpec as P

ROWS = 1024
SPAN = 128
MESH = pl.DeviceIdType.MESH
CHUNKS = 1
PAD = 8
GROUP = 16
LEVELS = 32767.0
TINY = 1e-30
VMEM_MOST = 67043328
VMEM_SPARE = 8 << 20


def encode(ids):
    level = jnp.zeros(ids.shape, jnp.int32)
    scale = jnp.ones(ids.shape, jnp.float32)
    for k in range(1, ROWS // SPAN):
        level = jnp.where(ids >= k * SPAN, k, level)
        scale = jnp.where(ids >= k * SPAN, float(1 << k), scale)
    return (ids - level * SPAN + SPAN).astype(jnp.float32) * scale


def powers(exps):
    return (
        1.0
        + (exps >= 1).astype(jnp.float32)
        + 2.0 * (exps >= 2).astype(jnp.float32)
        + 4.0 * (exps >= 3).astype(jnp.float32)
    )


def kernel(
    devs,
    pool,
    owner_hbm,
    x_hbm,
    ids_hbm,
    exps_hbm,
    acts_hbm,
    cot_hbm,
    table_ref,
    whole,
    bias_ref,
    xv,
    xs,
    idv,
    exv,
    codes,
    base,
    owner_ref,
    slots,
    send,
    recv,
    inter,
    ga,
    gc,
    oa,
    oc,
    part,
    yh,
    zbuf,
    bp,
    bh,
    bz,
    bx,
    coded,
    steps,
    lsem,
    psend,
    precv,
    csend,
    crecv,
    fsend,
    frecv,
    isend,
    irecv,
    ysend,
    yrecv,
    zsend,
    zrecv,
    bsend,
    brecv,
    gsend,
    grecv,
    esend,
    erecv,
):
    me = lax.axis_index("dev")
    grp = lax.axis_index("grp")
    other = 1 - grp
    samples, tables, feat = x_hbm.shape
    owned = table_ref.shape[0]
    id_rows = owned * pool
    zs = devs // 4
    core = lax.rem(me, 2)
    xbit = lax.rem(lax.div(me, 2), 2)
    z = lax.div(me, 4)
    place = lax.rem(me, 4)
    tall, wide = oa.shape[1], oc.shape[1]
    cols = wide // 128
    half = part.shape[0] // 2
    piece = half // zs
    pitch = samples + PAD

    def remote(src, dst, ssem, rsem, dev, group):
        return pltpu.make_async_remote_copy(
            src_ref=src,
            dst_ref=dst,
            send_sem=ssem,
            recv_sem=rsem,
            device_id={"grp": group, "dev": dev},
            device_id_type=MESH,
        )

    places = (
        place,
        place + 1 - 2 * core,
        place + 2 - 4 * xbit,
        place + 3 - 4 * xbit - 2 * core,
    )
    near = z * 4 + places[1]
    across = z * 4 + places[2]

    def columns(ref, part_index, width):
        return ref.at[:, pl.ds(pl.multiple_of(part_index * width, 128), width)]

    def slot_rows(ref, index):
        return ref.at[pl.ds(pl.multiple_of(index * samples, 8), samples)]

    owner_load = pltpu.make_async_copy(owner_hbm, owner_ref, lsem.at[6 + CHUNKS])
    owner_load.start()
    loads = [
        pltpu.make_async_copy(columns(acts_hbm, core, tall), slot_rows(ga, place), lsem.at[0]),
        pltpu.make_async_copy(columns(cot_hbm, xbit, wide), slot_rows(gc, place), lsem.at[1]),
        pltpu.make_async_copy(columns(acts_hbm, 1 - core, tall), oa, lsem.at[2]),
        pltpu.make_async_copy(columns(cot_hbm, 1 - xbit, wide), oc, lsem.at[3]),
        pltpu.make_async_copy(exps_hbm, exv, lsem.at[4]),
        pltpu.make_async_copy(ids_hbm, idv, lsem.at[5]),
    ]
    step = samples // CHUNKS
    for c in range(CHUNKS):
        span = pl.ds(c * step, step)
        loads.append(pltpu.make_async_copy(x_hbm.at[span], xv.at[span], lsem.at[6 + c]))
    for load in loads:
        load.start()

    barrier = pltpu.get_barrier_semaphore()

    def greet(dev, group):
        pl.semaphore_signal(
            barrier, inc=1, device_id={"grp": group, "dev": dev}, device_id_type=MESH
        )

    for m in range(1, 4):
        greet(z * 4 + places[m], grp)

    @pl.loop(1, zs)
    def _(k):
        greet(lax.rem(z + k, zs) * 4 + place, grp)

    greet(me, other)

    base[...] = (
        (lax.broadcasted_iota(jnp.int32, base.shape, 0) + SPAN)
        .astype(jnp.float32)
        .astype(jnp.bfloat16)
    )

    owner_load.wait()

    @pl.loop(0, tables)
    def _(k):
        slots[k] = lax.fori_loop(
            0,
            tables,
            lambda t, found: jnp.maximum(found, (owner_ref[t] == k).astype(jnp.int32) * t),
            jnp.int32(0),
            unroll=16,
        )

    pl.semaphore_wait(barrier, 3 + zs)

    def plane_copies(m, slot):
        acts = oa if m in (1, 3) else slot_rows(ga, place)
        cots = oc if m in (2, 3) else slot_rows(gc, place)
        who = z * 4 + places[m]
        return (
            remote(
                acts, slot_rows(ga, slot), isend.at[2 * m - 2], irecv.at[2 * m - 2], who, grp
            ),
            remote(
                cots, slot_rows(gc, slot), isend.at[2 * m - 1], irecv.at[2 * m - 1], who, grp
            ),
        )

    for load in loads[:4]:
        load.wait()
    for m in (2, 3, 1):
        for copy in plane_copies(m, place):
            copy.start()

    loads[4].wait()
    loads[5].wait()
    for p in range(pool):
        codes.reshape(tables * 8, samples)[pl.ds(p, tables, stride=8), :] = encode(idv[p])

    flat = xs.reshape(tables * pitch, feat)
    for c in range(CHUNKS):
        loads[6 + c].wait()

        @pl.loop(0, tables // GROUP)
        def _(g):
            some = pl.ds(pl.multiple_of(g * GROUP, GROUP), GROUP)
            factor = powers(exv[some, :])
            first = g * (GROUP * pitch)
            for k in range(c * step, (c + 1) * step):
                bound = jnp.broadcast_to(factor[:, k : k + 1], (GROUP, feat))
                value = xv[k, some, :].astype(jnp.float32)
                rows = pl.ds(first + k, GROUP, stride=pitch)
                flat[rows, :] = jnp.clip(value, -bound, bound)

    def build(target, dst):
        picked = []
        for s in range(owned):
            t = slots[dst * owned + s]
            target[pl.ds(s * samples, samples), :] = xs[t][:samples].astype(jnp.bfloat16)
            picked.append(codes[t][:pool])
        target[pl.ds(owned * samples, id_rows), :] = jnp.concatenate(picked, axis=0).astype(
            jnp.bfloat16
        )

    def each_near(act, first=1, last=zs):
        @pl.loop(first, last)
        def _(i):
            @pl.loop(0, 2)
            def _(j):
                peer = z + i * (1 - 2 * j)
                pl.when((peer >= 0) & (peer < zs))(functools.partial(act, peer))

    def close(act):
        each_near(act, 1, 2)

    def rest(act):
        each_near(act, 2, zs)

    def column_copy(m, peer):
        return remote(
            send.at[peer * 4 + places[m]],
            inter.at[m - 1, peer],
            psend.at[m - 1, peer],
            precv.at[m - 1, peer],
            z * 4 + places[m],
            grp,
        )

    def level_copy(m, back=False):
        who = z * 4 + places[m]
        return remote(
            send.at[who],
            recv.at[0, who if back else me],
            psend.at[m - 1, z],
            precv.at[m - 1, z],
            who,
            grp,
        )

    def line_copy(m, peer):
        origin = send.at[peer * 4 + place] if m == 0 else inter.at[m - 1, peer]
        return remote(
            origin,
            recv.at[0, z * 4 + places[m]],
            csend.at[m, peer],
            crecv.at[m, z],
            peer * 4 + place,
            grp,
        )

    def line_wait(m, peer):
        landing = recv.at[0, peer * 4 + places[m]]
        remote(
            landing, landing, csend.at[m, peer], crecv.at[m, peer], peer * 4 + place, grp
        ).wait_recv()

    def forward(src):
        return remote(
            recv.at[0, src], recv.at[1, src], fsend.at[src], frecv.at[src], me, other
        )

    def first_line(peer):
        dst = peer * 4 + place
        build(send.at[dst], dst)
        line_copy(0, peer).start()

    def column_start(m):
        def act(peer):
            dst = peer * 4 + places[m]
            build(send.at[dst], dst)
            column_copy(m, peer).start()

        each_near(act)

    def level_start(m):
        build(send.at[z * 4 + places[m]], z * 4 + places[m])
        level_copy(m).start()

    def column_pass(m, each):
        def act(peer):
            column_copy(m, peer).wait_recv()
            line_copy(m, peer).start()

        each(act)

    def level_pass(m):
        level_copy(m, True).wait_recv()
        forward(z * 4 + places[m]).start()

    def line_pass(m, each):
        def act(peer):
            line_wait(m, peer)
            forward(peer * 4 + places[m]).start()

        each(act)

    def plane_finish():
        for m in range(1, 4):
            for copy in plane_copies(m, places[m]):
                copy.wait_recv()
        bias = jnp.sum(gc[...].astype(jnp.float32), axis=0, keepdims=True)
        bp[0] = jnp.zeros(bp.shape[1:], jnp.float32)
        for j in range(cols):
            bp[0, j : j + 1, :] = bias[:, j * 128 : (j + 1) * 128]
        each = cols // 2
        for which in (other, grp):
            for j in range(each):
                block = which * each + j
                part[pl.ds(pl.multiple_of(block * tall, 8), tall), :] = lax.dot_general(
                    ga[...],
                    gc[:, pl.ds(pl.multiple_of(block * 128, 128), 128)],
                    (((0,), (0,)), ((), ())),
                    preferred_element_type=jnp.float32,
                )
            if which is other:
                y_start()

    def y_copies():
        away = part.at[pl.ds(pl.multiple_of(other * half, 8), half)]
        return (
            remote(away, yh, ysend.at[0], yrecv.at[0], me, other),
            remote(bp.at[0], bh, ysend.at[1], yrecv.at[1], me, other),
        )

    def y_start():
        for copy in y_copies():
            copy.start()

    def y_finish():
        for copy in y_copies():
            copy.wait_recv()
        keep = pl.ds(pl.multiple_of(grp * half, 8), half)
        part[keep, :] = part[keep, :] + yh[...]
        bp[1] = bp[0] + bh[...]

    def piece_of(peer):
        return pl.ds(pl.multiple_of(grp * half + peer * piece, 8), piece)

    def z_copy(k, back=False):
        peer = lax.rem(z + k, zs)
        dev = peer * 4 + place
        origin, landing = (z, peer) if back else (peer, z)
        return (
            remote(
                part.at[piece_of(origin)],
                zbuf.at[landing],
                zsend.at[peer],
                zrecv.at[landing],
                dev,
                grp,
            ),
            remote(bp.at[1], bz.at[landing], bsend.at[peer], brecv.at[landing], dev, grp),
        )

    def z_start():
        @pl.loop(1, zs)
        def _(k):
            for copy in z_copy(k):
                copy.start()

    def z_finish():
        zbuf[z] = part[piece_of(z), :]
        bz[z] = bp[1]

        @pl.loop(1, zs)
        def _(k):
            for copy in z_copy(k, True):
                copy.wait_recv()

        total = lax.fori_loop(1, zs, lambda i, run: run + zbuf[i], zbuf[0])
        top = jnp.maximum(jnp.max(jnp.abs(total), axis=0, keepdims=True), TINY)
        coded[place, grp, z] = jnp.round(total * (LEVELS / top)).astype(jnp.int32).astype(jnp.int16)
        steps[place, grp, z] = top * (1.0 / LEVELS)
        bp[2] = lax.fori_loop(1, zs, lambda i, run: run + bz[i], bz[0])

    def zg_copy(k, back=False):
        peer = lax.rem(z + k, zs)
        dev = peer * 4 + place
        origin = peer if back else z
        return [
            remote(ref.at[place, grp, origin], ref.at[place, grp, origin], ss, rs, dev, grp)
            for ref, ss, rs in (
                (coded, gsend.at[0, peer], grecv.at[0, origin]),
                (steps, gsend.at[1, peer], grecv.at[1, origin]),
            )
        ]

    def bias_copy():
        return remote(bp.at[2], bx, bsend.at[zs], brecv.at[zs], across, grp)

    def zg_start():
        @pl.loop(1, zs)
        def _(k):
            for copy in zg_copy(k):
                copy.start()

        bias_copy().start()

    def zg_finish():
        @pl.loop(1, zs)
        def _(k):
            for copy in zg_copy(k, True):
                copy.wait_recv()

    halves = (grp, other)

    def gather_copy(k, back=False):
        if k == 0:
            tile, which, dev, group = place, other if back else grp, me, other
        elif k < 3:
            tile, which, dev, group = places[2] if back else place, halves[k - 1], across, grp
        elif k < 5:
            tile, which, dev, group = places[1] if back else place, halves[k - 3], near, grp
        else:
            tile = places[3] if back else places[2]
            which, dev, group = halves[k - 5], near, grp
        return [
            remote(
                ref.at[tile, which], ref.at[tile, which], esend.at[i, k], erecv.at[i, k], dev, group
            )
            for i, ref in enumerate((coded, steps))
        ]

    def gather_start(*ks):
        for k in ks:
            for copy in gather_copy(k):
                copy.start()

    def gather_wait(*ks):
        for k in ks:
            for copy in gather_copy(k, True):
                copy.wait_recv()

    def decode(tile, which):
        @pl.loop(0, zs)
        def _(i):
            code = coded[tile, which, i].astype(jnp.int32).astype(jnp.float32)
            rows = pl.ds(pl.multiple_of(which * half + i * piece, 8), piece)
            whole[tile, rows, :] = code * steps[tile, which, i]

    def accumulate(side, first, second):
        marks = jnp.concatenate(
            [
                recv[side, c, pl.ds(owned * samples, id_rows), :].astype(jnp.float32)
                for c in (first, second)
            ],
            axis=1,
        )
        one, zero = jnp.bfloat16(1), jnp.bfloat16(0)
        axis = base[...]
        for s in range(owned):
            values = jnp.concatenate(
                [recv[side, c, pl.ds(s * samples, samples), :] for c in (first, second)],
                axis=0,
            )
            rows = marks[s * pool : (s + 1) * pool]
            for block in range(ROWS // SPAN):
                local = (rows * (1.0 / (1 << block))).astype(jnp.bfloat16)
                counts = jnp.where(local[0:1] == axis, one, zero)
                for p in range(1, pool):
                    counts = counts + jnp.where(local[p : p + 1] == axis, one, zero)
                span = pl.ds(block * SPAN, SPAN)
                table_ref[s, span, :] = table_ref[s, span, :] + jnp.dot(
                    counts, values, preferred_element_type=jnp.float32
                )

    def pair(side, part_of, peer):
        accumulate(side, peer * 4 + places[2 * part_of], peer * 4 + places[2 * part_of + 1])

    def far_pair(part_of, peer):
        for m in (2 * part_of, 2 * part_of + 1):
            forward(peer * 4 + places[m]).wait_recv()
        pair(1, part_of, peer)

    each_near(first_line)
    build(recv.at[0, me], me)
    forward(me).start()
    level_start(1)
    column_start(2)
    level_start(2)
    level_start(3)
    column_start(1)
    column_start(3)
    column_pass(1, close)
    plane_finish()
    column_pass(1, rest)
    level_pass(1)
    table_ref[...] = jnp.zeros(table_ref.shape, jnp.float32)
    line_pass(0, close)
    y_finish()
    z_start()
    level_pass(2)
    level_pass(3)
    line_pass(0, rest)
    column_pass(2, close)
    pair(0, 0, z)
    line_pass(1, close)
    z_finish()
    zg_start()
    column_pass(2, rest)
    line_pass(1, rest)
    zg_finish()
    gather_start(0, 1, 3)
    column_pass(3, close)
    column_pass(3, rest)
    close(functools.partial(pair, 0, 0))
    rest(functools.partial(pair, 0, 0))
    far_pair(0, z)
    line_pass(2, close)
    line_pass(2, rest)
    pair(0, 1, z)
    close(functools.partial(far_pair, 0))
    gather_wait(0)
    gather_start(2, 4)
    decode(place, grp)
    decode(place, other)
    rest(functools.partial(far_pair, 0))
    line_pass(3, close)
    line_pass(3, rest)
    gather_wait(1)
    gather_start(5)
    decode(places[2], grp)
    close(functools.partial(pair, 0, 1))
    rest(functools.partial(pair, 0, 1))
    far_pair(1, z)
    gather_wait(2)
    gather_start(6)
    decode(places[2], other)
    close(functools.partial(far_pair, 1))
    rest(functools.partial(far_pair, 1))
    gather_wait(3, 4)
    decode(places[1], grp)
    decode(places[1], other)
    gather_wait(5, 6)
    decode(places[3], grp)
    decode(places[3], other)

    bias_copy().wait_recv()
    mine, theirs = bp[2], bx[...]
    lower = jnp.where(xbit == 0, mine, theirs)
    upper = jnp.where(xbit == 0, theirs, mine)
    for j in range(cols):
        bias_ref[:, j * 128 : (j + 1) * 128] = lower[j : j + 1, :]
        bias_ref[:, (cols + j) * 128 : (cols + j + 1) * 128] = upper[j : j + 1, :]

    bias_copy().wait_send()
    for copy in y_copies():
        copy.wait_send()
    for k in range(7):
        for copy in gather_copy(k):
            copy.wait_send()
    for m in range(1, 4):
        level_copy(m).wait_send()
        for copy in plane_copies(m, place):
            copy.wait_send()

    @pl.loop(1, zs)
    def _(k):
        for copy in z_copy(k):
            copy.wait_send()
        for copy in zg_copy(k):
            copy.wait_send()

    def drain(peer):
        for m in range(4):
            line_copy(m, peer).wait_send()
            if m > 0:
                column_copy(m, peer).wait_send()

    each_near(drain)

    @pl.loop(0, devs)
    def _(src):
        forward(src).wait_send()


def place_outputs(table_in, whole_in, bias_in, table_out, weight_out, bias_out, sems):
    tiles, rows, _ = whole_in.shape
    tall = weight_out.shape[0] // 2
    cols = rows // tall
    copies = []
    for s in range(table_in.shape[0]):
        copies.append((table_in.at[s], table_out.at[s]))
    for tile in range(tiles):
        for j in range(cols):
            block = (tile // 2) * cols + j
            copies.append(
                (
                    whole_in.at[tile, pl.ds(j * tall, tall)],
                    weight_out.at[pl.ds((tile % 2) * tall, tall), pl.ds(block * 128, 128)],
                )
            )
    copies.append((bias_in, bias_out))
    started = [
        pltpu.make_async_copy(src, dst, sems.at[i]) for i, (src, dst) in enumerate(copies)
    ]
    for copy in started:
        copy.start()
    for copy in started:
        copy.wait()


def solution(mesh):
    devs = mesh.shape["dev"]

    def per_device(pooled_grad, row_ids, scale_exps, table_owner, dense_acts, dense_cot):
        samples, tables, feat = pooled_grad.shape
        pool = row_ids.shape[1]
        owned = tables // devs
        hid, hid2 = dense_acts.shape[1], dense_cot.shape[1]
        tall, wide = hid // 2, hid2 // 2
        zs = devs // 4
        rows = owned * (samples + pool)
        total = tall * wide // 128
        half = total // 2
        dma = pltpu.SemaphoreType.DMA
        vmem = pl.BlockSpec(memory_space=pltpu.VMEM)
        hbm = pl.BlockSpec(memory_space=pltpu.HBM)
        f32, bf16, i32 = jnp.float32, jnp.bfloat16, jnp.int32
        buffers = [
            pltpu.VMEM((samples, tables, feat), bf16),
            pltpu.VMEM((tables, samples + PAD, feat), f32),
            pltpu.VMEM((pool, tables, samples), i32),
            pltpu.VMEM((tables, samples), i32),
            pltpu.VMEM((tables, 8, samples), f32),
            pltpu.VMEM((SPAN, 2 * samples), bf16),
            pltpu.VMEM((devs, rows, feat), bf16),
            pltpu.VMEM((2, devs, rows, feat), bf16),
            pltpu.VMEM((3, zs, rows, feat), bf16),
            pltpu.VMEM((4 * samples, tall), bf16),
            pltpu.VMEM((4 * samples, wide), bf16),
            pltpu.VMEM((samples, tall), bf16),
            pltpu.VMEM((samples, wide), bf16),
            pltpu.VMEM((total, 128), f32),
            pltpu.VMEM((half, 128), f32),
            pltpu.VMEM((zs, half // zs, 128), f32),
            pltpu.VMEM((3, 8, 128), f32),
            pltpu.VMEM((8, 128), f32),
            pltpu.VMEM((zs, 8, 128), f32),
            pltpu.VMEM((8, 128), f32),
            pltpu.VMEM((4, 2, zs, half // zs, 128), jnp.int16),
            pltpu.VMEM((4, 2, zs, 1, 128), f32),
        ]
        held = sum(math.prod(b.shape) * jnp.dtype(b.dtype).itemsize for b in buffers)
        partial = pl.pallas_call(
            functools.partial(kernel, devs, pool),
            out_shape=(
                jax.ShapeDtypeStruct((owned, ROWS, feat), f32),
                jax.ShapeDtypeStruct((4, total, 128), f32),
                jax.ShapeDtypeStruct((1, hid2), f32),
            ),
            in_specs=[hbm] * 6,
            out_specs=(vmem, vmem, vmem),
            scratch_shapes=buffers[:6]
            + [pltpu.SMEM((tables,), i32)] * 2
            + buffers[6:]
            + [
                dma((7 + CHUNKS,)),
                dma((3, zs)),
                dma((3, zs)),
                dma((4, zs)),
                dma((4, zs)),
                dma((devs,)),
                dma((devs,)),
                dma((6,)),
                dma((6,)),
                dma((2,)),
                dma((2,)),
                dma((zs,)),
                dma((zs,)),
                dma((zs + 1,)),
                dma((zs + 1,)),
                dma((2, zs)),
                dma((2, zs)),
                dma((2, 7)),
                dma((2, 7)),
            ],
            compiler_params=pltpu.CompilerParams(
                collective_id=0,
                has_side_effects=True,
                vmem_limit_bytes=min(held + VMEM_SPARE, VMEM_MOST),
            ),
        )(
            pltpu.with_memory_space_constraint(table_owner, pltpu.HBM),
            pltpu.with_memory_space_constraint(pooled_grad, pltpu.HBM),
            pltpu.with_memory_space_constraint(jnp.transpose(row_ids, (1, 2, 0)), pltpu.HBM),
            pltpu.with_memory_space_constraint(jnp.transpose(scale_exps, (1, 0)), pltpu.HBM),
            pltpu.with_memory_space_constraint(dense_acts, pltpu.HBM),
            pltpu.with_memory_space_constraint(dense_cot, pltpu.HBM),
        )
        cols = total // tall
        table_grad, weight_grad, bias_grad = pl.pallas_call(
            place_outputs,
            out_shape=(
                jax.ShapeDtypeStruct((owned, ROWS, feat), f32),
                jax.ShapeDtypeStruct((hid, hid2), f32),
                jax.ShapeDtypeStruct((1, hid2), f32),
            ),
            in_specs=[vmem] * 3,
            out_specs=(hbm, hbm, hbm),
            scratch_shapes=[dma((owned + 4 * cols + 1,))],
            compiler_params=pltpu.CompilerParams(vmem_limit_bytes=16 << 20),
        )(*partial)
        return table_grad, weight_grad, bias_grad.reshape(hid2)

    return jax.shard_map(
        per_device,
        mesh=mesh,
        in_specs=(
            P(("grp", "dev"), None, None),
            P(("grp", "dev"), None, None),
            P(("grp", "dev"), None),
            P(),
            P(("grp", "dev"), None),
            P(("grp", "dev"), None),
        ),
        out_specs=(P("dev", None, None), P(), P()),
        check_vma=False,
    )
```
